32 devices in a mesh: cfg: 4 (over z), tm: 8 (over y, x, core).
Axes of the slice: x: 2, y: 2, z: 4, core: 2. Of those that a mesh axis runs over, the one named last changes fastest.
Arguments:
- linv: bfloat16 [16384, 1024], P(('cfg', 'tm')), parts along dimension 0, as said below
- sub: bfloat16 [16384, 1024], P(('cfg', 'tm')), parts along dimension 0, may hold values from -0.046875 to 0.046875
- owner: int32 [16], P('cfg'), parts along dimension 0, may hold values from 0 to 7, as said below
Outputs:
- diag_cov: bfloat16 [16384, 1024], P(('cfg', 'tm')), parts along dimension 0
- off_cov: bfloat16 [16384, 1024], P(('cfg', 'tm')), parts along dimension 0
- owned_var: float32 [64, 1024], P(('cfg', 'tm')), parts along dimension 0
The draws below stay inside these ranges and needn't reach their ends.
There are 4 independent parts, one for each index of `cfg`. The reference program is written for one: setup_inputs(seed, part) draws one part's arguments, and reference() takes and returns one part's arrays. A program takes and returns all parts, laid end to end along the dimension named above; each array names one. Nothing has to cross between parts.
Inputs may be any that keep to these rules, and one draw needn't show every extreme that they name: Each block of 1024 rows of linv is lower triangular with a positive diagonal. Exactly two time blocks, adjacent in time, share an owner; all other time blocks have distinct owners, so no owner receives more than 2 blocks and one receives exactly 2.
All inputs are finite; a program needn't handle non-finite values.
Results may differ from the reference program's by a relative error of at most 0.0075.
Values may be sent and summed in bfloat16 or wider, within the bound.
No kernel may reach another device: no remote copies, remote signals or barrier semaphores. Data moves between devices by JAX's collectives and lax.ppermute only.
A program may use at most 64 MiB of HBM per device.

```python
import math
import jax
import jax.numpy as jnp
from jax import lax

B = 1024
TB = 4
SLOTS = 2
N_TM = 8


def lower_factor(factor_key):
    diag_key, low_key = jax.random.split(factor_key, 2)
    diagonal_part = jnp.exp(jax.random.uniform(diag_key, (B,), jnp.float32, math.log(0.6), math.log(1.8)))
    spread = jax.random.normal(low_key, (B, B), jnp.float32)
    lower_part = jnp.tril(spread, -1) * (0.5 / math.sqrt(B))
    return lower_part + jnp.diag(diagonal_part)


def draw_linv(key, part):
    factor_keys = jax.random.split(jax.random.fold_in(key, 11), TB)
    stacked = jax.vmap(lower_factor)(factor_keys)
    return stacked.reshape(TB * B, B).astype(jnp.bfloat16)


def draw_sub(key, part):
    sub_key = jax.random.fold_in(key, 37)
    edge_bound = 1.5 / math.sqrt(B)
    values = jnp.clip(jax.random.normal(sub_key, (TB * B, B), jnp.float32) * (0.8 / math.sqrt(B)), -edge_bound, edge_bound)
    return values.astype(jnp.bfloat16)


def draw_owner(key, part):
    perm_key, pair_key = jax.random.split(jax.random.fold_in(key, 23))
    order_perm = jax.random.permutation(perm_key, N_TM)
    pair_at = jax.random.randint(pair_key, (), 0, TB - 1)
    steps_iota = jnp.arange(TB, dtype=jnp.int32)
    picked = jnp.where(steps_iota <= pair_at, steps_iota, steps_iota - 1)
    return order_perm[picked].astype(jnp.int32)


def setup_inputs(seed: int = 0, part: int = 0) -> dict:
    key_of = jax.random.split(jax.random.key(seed), 4)
    part_keys = jax.random.split(jax.random.fold_in(key_of[3], part), 4)
    linv = draw_linv(jax.random.fold_in(jax.random.fold_in(key_of[3], part), 71), part)
    sub = draw_sub(jax.random.fold_in(jax.random.fold_in(key_of[3], part), 71), part)
    owner = draw_owner(jax.random.fold_in(jax.random.fold_in(key_of[3], part), 71), part)
    return {"linv": linv, "sub": sub, "owner": owner}


def reference(linv, sub, owner):
    contract_first = (((0,), (0,)), ((), ()))
    identity = jnp.eye(B, dtype=jnp.bfloat16)
    carried = identity
    diag_parts = []
    off_parts = []
    for step_index in range(TB - 1, -1, -1):
        factor = linv[step_index * B:(step_index + 1) * B]
        lower_block = sub[step_index * B:(step_index + 1) * B]
        coupling = jnp.dot(lower_block, factor, preferred_element_type=jnp.float32).astype(jnp.bfloat16)
        gram = lax.dot_general(factor, factor, contract_first, preferred_element_type=jnp.float32)
        off_block = (-jnp.dot(carried, coupling, preferred_element_type=jnp.float32)).astype(jnp.bfloat16)
        diag_block = (gram - lax.dot_general(coupling, off_block, contract_first, preferred_element_type=jnp.float32)).astype(jnp.bfloat16)
        diag_parts.insert(0, diag_block)
        off_parts.insert(0, off_block)
        carried = diag_block
    diag_cov = jnp.concatenate(diag_parts, 0)
    off_cov = jnp.concatenate(off_parts, 0)
    variances = jnp.stack([jnp.diagonal(entry_block).astype(jnp.float32) for entry_block in diag_parts])
    positions = jnp.arange(TB, dtype=jnp.int32)
    same_owner = owner[:, None] == owner[None, :]
    earlier = positions[None, :] < positions[:, None]
    slot_rank = jnp.sum(jnp.where(same_owner & earlier, 1, 0).astype(jnp.int32), axis=1).astype(jnp.int32)
    target = (owner * SLOTS + slot_rank).astype(jnp.int32)
    owned_var = jnp.zeros((N_TM * SLOTS, B), jnp.float32).at[target].set(variances)
    return diag_cov, off_cov, owned_var
```

```python
import jax
import jax.numpy as jnp
from jax import lax
from jax.sharding import PartitionSpec as P

TB = 4
SLOTS = 2
SPARE = 8

CONTRACT_FIRST = (((0,), (0,)), ((), ()))
BF16 = jnp.bfloat16
F32 = jnp.float32


def mm(a, b):
    return jnp.dot(a, b, preferred_element_type=F32)


def mm_t(a, b):
    return lax.dot_general(a, b, CONTRACT_FIRST, preferred_element_type=F32)


def shards(linv, sub, owner):
    group = lax.axis_size("tm") // TB
    rows, n = linv.shape
    half = n // 2
    paired = group == 2
    dev = lax.axis_index("tm")
    member = dev % group
    block = dev // group
    start = member * rows

    def block_to_block(values, source, target, members=range(group)):
        pairs = [(source * group + i, target * group + i) for i in members]
        return lax.ppermute(values, "tm", pairs)

    def gather(piece):
        step = 1
        while step < group:
            route = [(i, i ^ step) for i in range(TB * group)]
            other = lax.ppermute(piece, "tm", route)
            upper = (member // step) % 2 == 1
            piece = jnp.concatenate(
                [jnp.where(upper, other, piece), jnp.where(upper, piece, other)], 0
            )
            step *= 2
        return piece

    def gather_stacked(piece):
        return gather(piece[None])

    def own_cols(full):
        return lax.dynamic_slice_in_dim(full, start, rows, 1)

    def diagonal(square):
        size = square.shape[0]
        r = lax.broadcasted_iota(jnp.int32, (size, size), 0)
        c = lax.broadcasted_iota(jnp.int32, (size, size), 1)
        return jnp.sum(jnp.where(r == c, square.astype(F32), 0.0), axis=0)

    if paired:
        r_iota = lax.broadcasted_iota(jnp.int32, (rows, rows), 0)
        c_iota = lax.broadcasted_iota(jnp.int32, (rows, rows), 1)

    def pack(own_rows, passenger):
        if not paired:
            spare = jnp.zeros((SPARE, n), BF16).at[0].set(passenger.astype(BF16))
            return jnp.concatenate([own_rows, spare], 0)
        mine = lax.dynamic_slice_in_dim(own_rows, start, rows, 1)
        cross = lax.dynamic_slice_in_dim(own_rows, rows - start, rows, 1)
        body = jnp.where(c_iota >= r_iota, mine, cross)
        spare = jnp.concatenate(
            [
                diagonal(cross)[None],
                passenger.reshape(2, rows),
                jnp.zeros((SPARE - 3, rows), F32),
            ],
            0,
        ).astype(BF16)
        return jnp.concatenate([body, spare], 0)

    def unpack(packet):
        if not paired:
            full = gather(packet[:rows])
            return full, diagonal(full), packet[rows].astype(F32)
        both = gather_stacked(packet)
        p0 = both[0, :rows]
        p1 = both[1, :rows]
        p0t = p0.T
        p1t = p1.T
        on_cross = both[0, rows][None, :]
        s00 = jnp.where(c_iota >= r_iota, p0, p0t)
        s11 = jnp.where(c_iota >= r_iota, p1, p1t)
        s01 = jnp.where(c_iota < r_iota, p0, jnp.where(c_iota > r_iota, p1t, on_cross))
        s10 = jnp.where(c_iota > r_iota, p0t, jnp.where(c_iota < r_iota, p1, on_cross))
        full = jnp.concatenate(
            [jnp.concatenate([s00, s01], 1), jnp.concatenate([s10, s11], 1)], 0
        )
        diag = jnp.concatenate([diagonal(p0), diagonal(p1)])
        passenger = both[0, rows + 1 : rows + 3].astype(F32).reshape(n)
        return full, diag, passenger

    sub_1 = block_to_block(sub, 1, 0)
    left_1 = block_to_block(linv[:, :half], 1, 0)
    right_1 = block_to_block(linv[:, half:], 1, 0, range(group // 2, group))

    factor = gather(linv)
    lower = gather(sub)
    coupling = mm(lower, factor).astype(BF16)
    gram_rows = mm_t(own_cols(factor), factor)
    gram_diag = jnp.sum(jnp.square(factor.astype(F32)), axis=0)
    coupling_cols = own_cols(coupling)
    off_3 = -lax.dynamic_slice_in_dim(coupling, start, rows, 0)
    cov_3 = (gram_rows + mm_t(coupling_cols, coupling)).astype(BF16)

    packet = block_to_block(pack(cov_3, jnp.zeros((n,), F32)), 3, 2)
    carried, var_3, _ = unpack(packet)
    off_2_full = (-mm(carried, coupling)).astype(BF16)
    off_2 = lax.dynamic_slice_in_dim(off_2_full, start, rows, 0)
    cov_2 = (gram_rows - mm_t(coupling_cols, off_2_full)).astype(BF16)

    packet = pack(cov_2, var_3)
    packet_0 = block_to_block(packet, 2, 0)
    packet_1 = block_to_block(packet, 2, 1)

    at_first = block == 0
    factor_1 = gather(jnp.where(at_first, jnp.concatenate([left_1, right_1], 1), linv))
    lower_1 = gather(jnp.where(at_first, sub_1, sub))
    coupling_1 = mm(lower_1, factor_1).astype(BF16)
    gram_1 = mm_t(factor_1, factor_1)

    carried, var_2, var_3 = unpack(jnp.where(at_first, packet_0, packet_1))
    off_1_full = (-mm(carried, coupling_1)).astype(BF16)
    cov_1_full = (gram_1 - mm_t(coupling_1, off_1_full)).astype(BF16)
    off_1 = lax.dynamic_slice_in_dim(off_1_full, start, rows, 0)
    cov_1 = lax.dynamic_slice_in_dim(cov_1_full, start, rows, 0)
    var_1 = diagonal(cov_1_full)

    off_0_full = (-mm(cov_1_full, coupling)).astype(BF16)
    off_0 = lax.dynamic_slice_in_dim(off_0_full, start, rows, 0)
    var_0 = gram_diag - jnp.sum(coupling.astype(F32) * off_0_full.astype(F32), axis=0)
    cov_0 = (gram_rows - mm_t(coupling_cols, off_0_full)).astype(BF16)

    variances = jnp.stack([var_0, var_1, var_2, var_3]).astype(BF16)
    heard = [block_to_block(variances, 0, t) for t in range(1, TB)]
    variances = jnp.where(at_first, variances, sum(heard)).astype(F32)

    def choose(at_0, at_1, at_2, at_3):
        late = jnp.where(at_first, at_0, at_1)
        return jnp.where(block < 2, late, jnp.where(block == 2, at_2, at_3))

    cov_rows = choose(cov_0, cov_1, cov_2, cov_3)
    off_rows = choose(off_0, off_1, off_2, off_3)

    positions = lax.broadcasted_iota(jnp.int32, (TB, TB), 1)
    current = lax.broadcasted_iota(jnp.int32, (TB, TB), 0)
    same_owner = owner[:, None] == owner[None, :]
    slot_rank = jnp.sum(jnp.where(same_owner & (positions < current), 1, 0), axis=1)
    slot_iota = lax.broadcasted_iota(jnp.int32, (SLOTS, TB), 0)
    selector = (owner[None, :] == dev) & (slot_rank[None, :] == slot_iota)
    owned_var = sum(
        jnp.where(selector[:, t, None], variances[t][None, :], 0.0) for t in range(TB)
    )
    return (cov_rows, off_rows, owned_var)


def solution(mesh):
    return jax.shard_map(
        shards,
        mesh=mesh,
        in_specs=(P(("cfg", "tm"), None), P(("cfg", "tm"), None), P("cfg")),
        out_specs=(P(("cfg", "tm"), None), P(("cfg", "tm"), None), P(("cfg", "tm"), None)),
        check_vma=False,
    )
```

```python
import functools

import jax
import jax.numpy as jnp
from jax import lax
from jax.experimental import pallas as pl
from jax.experimental.pallas import tpu as pltpu
from jax.sharding import PartitionSpec as P

TB = 4
SLOTS = 2
SPARE = 16
TILE = 128

CONTRACT_FIRST = (((0,), (0,)), ((), ()))
BF16 = jnp.bfloat16
F32 = jnp.float32

ANY = pl.BlockSpec(memory_space=pl.ANY)
VMEM = pl.BlockSpec(memory_space=pltpu.VMEM)
SMEM = pl.BlockSpec(memory_space=pltpu.SMEM)
PARAMS = pltpu.CompilerParams(vmem_limit_bytes=36 << 20)


def mm(a, b):
    return jnp.dot(a, b, preferred_element_type=F32)


def mm_t(a, b):
    return lax.dot_general(a, b, CONTRACT_FIRST, preferred_element_type=F32)


def iotas(size):
    r = lax.broadcasted_iota(jnp.int32, (size, size), 0)
    c = lax.broadcasted_iota(jnp.int32, (size, size), 1)
    return r, c


def load_rows(target, pieces, start, sems):
    n = target.shape[0]
    if len(pieces) == 1:
        copies = [pltpu.make_async_copy(pieces[0], target, sems.at[0])]
    else:
        rows = pieces[0].shape[0]
        other = n - rows - start
        copies = [
            pltpu.make_async_copy(pieces[0], target.at[pl.ds(start, rows)], sems.at[0]),
            pltpu.make_async_copy(pieces[1], target.at[pl.ds(other, rows)], sems.at[1]),
        ]
    for copy in copies:
        copy.start()
    return copies


def couple(target, lower, factor):
    n = factor.shape[0]
    half = n // 2
    target[:, :half] = mm(lower[...], factor[:, :half]).astype(BF16)
    target[:, half:] = mm(lower[:, half:], factor[half:, half:]).astype(BF16)


def tile_diag(tile):
    r, c = iotas(TILE)
    return jnp.sum(jnp.where(r == c, tile.astype(F32), 0.0), axis=0, keepdims=True)


def pack(packet, cov, start, passenger, paired):
    rows, n = cov.shape
    row = lax.broadcasted_iota(jnp.int32, (SPARE, n if not paired else rows), 0)
    if not paired:
        packet[:rows, :] = cov[...]
        packet[rows:, :] = jnp.where(row == 0, passenger, 0.0).astype(BF16)
        return
    other = n - rows - start
    r, c = iotas(TILE)
    for i in range(0, rows, TILE):
        for j in range(0, rows, TILE):
            mine = cov[i : i + TILE, pl.ds(pl.multiple_of(start + j, TILE), TILE)]
            cross = cov[i : i + TILE, pl.ds(pl.multiple_of(other + j, TILE), TILE)]
            if j > i:
                tile = mine
            elif j < i:
                tile = cross
            else:
                tile = jnp.where(c >= r, mine.astype(F32), cross.astype(F32)).astype(BF16)
                dx = tile_diag(cross)
                spare = jnp.where(row[:, :TILE] == 0, dx, 0.0)
                for k in range(n // rows):
                    at = k * rows + i
                    spare = jnp.where(
                        row[:, :TILE] == k + 1, passenger[:, at : at + TILE], spare
                    )
                packet[rows:, i : i + TILE] = spare.astype(BF16)
            packet[i : i + TILE, j : j + TILE] = tile


def unpack(full, diag, packets, start, paired):
    n = full.shape[0]
    if not paired:
        (packet,) = packets
        rows = packet.shape[1] - SPARE
        for k in range(packet.shape[0]):
            full[k * rows : (k + 1) * rows, :] = packet[k, :rows, :]
        for i in range(0, n, TILE):
            diag[:, i : i + TILE] = tile_diag(full[i : i + TILE, i : i + TILE])
        return packet[0, rows:, :].astype(F32)[0:1]
    rows = packets[0].shape[0] - SPARE
    base = (start, n - rows - start)
    r, c = iotas(TILE)

    def put(at_row, i, at_col, j, tile):
        full[
            pl.ds(pl.multiple_of(at_row + i, TILE), TILE),
            pl.ds(pl.multiple_of(at_col + j, TILE), TILE),
        ] = tile

    spare = packets[0][rows:, :].astype(F32)
    for mine, yours in ((0, 1), (1, 0)):
        for i in range(0, rows, TILE):
            for j in range(0, rows, TILE):
                tile = packets[mine][i : i + TILE, j : j + TILE]
                flip = tile.T
                if j > i:
                    put(base[mine], i, base[mine], j, tile)
                    put(base[mine], j, base[mine], i, flip)
                elif j < i:
                    put(base[mine], i, base[yours], j, tile)
                    put(base[yours], j, base[mine], i, flip)
                else:
                    tile = tile.astype(F32)
                    flip = flip.astype(F32)
                    theirs = packets[yours][i : i + TILE, i : i + TILE].T.astype(F32)
                    own = jnp.where(c >= r, tile, flip)
                    put(base[mine], i, base[mine], i, own.astype(BF16))
                    dx = spare[0:1, i : i + TILE]
                    cross = jnp.where(c < r, tile, jnp.where(c > r, theirs, dx))
                    put(base[mine], i, base[yours], i, cross.astype(BF16))
                    diag[:, pl.ds(pl.multiple_of(base[mine] + i, TILE), TILE)] = tile_diag(own)
    return jnp.concatenate([spare[k + 1 : k + 2] for k in range(n // rows)], 1)


def first_kernel(pieces, paired, ids, *refs):
    factors, lowers = refs[:pieces], refs[pieces : 2 * pieces]
    coupling, packet, cov, factor, lower, total, sems = refs[2 * pieces :]
    rows = cov.shape[0]
    start = pl.multiple_of(ids[0], rows)
    block = ids[1]
    copies = load_rows(factor, factors, start, sems.at[0])
    copies += load_rows(lower, lowers, start, sems.at[1])
    for copy in copies:
        copy.wait()
    couple(coupling, lower, factor)

    @pl.when(block == TB - 1)
    def _():
        own = pl.ds(start, rows)
        total[...] = mm_t(factor[:, own], factor[...])
        cov[...] = (total[...] + mm_t(coupling[:, own], coupling[...])).astype(BF16)
        pack(packet, cov, start, jnp.zeros((1, factor.shape[1]), F32), paired)


def gram_kernel(pieces, ids, *refs):
    factors = refs[:pieces]
    coupling, cov, gram, off_out, cov_out, factor, off, sems, out_sems = refs[pieces:]
    rows = cov.shape[0]
    start = pl.multiple_of(ids[0], rows)
    block = ids[1]
    copies = load_rows(factor, factors, start, sems.at[0])
    for copy in copies:
        copy.wait()
    gram[...] = mm_t(factor[:, pl.ds(start, rows)], factor[...])

    @pl.when(block == TB - 1)
    def _():
        off[...] = -coupling[pl.ds(start, rows), :]
        one = pltpu.make_async_copy(off, off_out, out_sems.at[0])
        two = pltpu.make_async_copy(cov, cov_out, out_sems.at[1])
        one.start()
        two.start()
        one.wait()
        two.wait()


def second_kernel(pieces, paired, ids, *refs):
    packets = refs[:pieces]
    coupling, gram, packet, off, cov, full, diag = refs[pieces:]
    rows = cov.shape[0]
    start = pl.multiple_of(ids[0], rows)
    block = ids[1]

    @pl.when(block == TB - 2)
    def _():
        unpack(full, diag, packets, start, paired)
        off[...] = (-mm(full[...], coupling[...])).astype(BF16)
        cov[...] = (gram[...] - mm_t(coupling[:, pl.ds(start, rows)], off[...])).astype(BF16)
        pack(packet, cov, start, diag[...], paired)


def ready_kernel(pieces, ids, *refs):
    factors, heard_factors = refs[:pieces], refs[pieces : 2 * pieces]
    heard_lowers = refs[2 * pieces : 3 * pieces]
    (coupling, off, cov, _, _, coupling_1, gram_1, coupling_0, diag_0, off_out, cov_out,
     factor, heard, lower, sems, out_sems) = refs[3 * pieces :]
    rows = cov.shape[0]
    start = pl.multiple_of(ids[0], rows)
    block = ids[1]

    @pl.when(block == TB - 2)
    def _():
        one = pltpu.make_async_copy(off.at[pl.ds(start, rows)], off_out, out_sems.at[0])
        two = pltpu.make_async_copy(cov, cov_out, out_sems.at[1])
        one.start()
        two.start()
        one.wait()
        two.wait()

    @pl.when(block < 2)
    def _():
        copies = load_rows(factor, factors, start, sems.at[0])
        copies += load_rows(heard, heard_factors, start, sems.at[1])
        copies += load_rows(lower, heard_lowers, start, sems.at[2])
        for copy in copies:
            copy.wait()

        def finish(factor_1, factor_0):
            gram_1[...] = mm_t(factor_1[...], factor_1[...])
            diag_0[...] = jnp.sum(
                jnp.square(factor_0[...].astype(F32)), axis=0, keepdims=True
            )

        @pl.when(block == 0)
        def _():
            couple(coupling_1, lower, heard)
            coupling_0[...] = coupling[...]
            finish(heard, factor)

        @pl.when(block == 1)
        def _():
            couple(coupling_0, lower, heard)
            coupling_1[...] = coupling[...]
            finish(factor, heard)


def third_kernel(pieces, paired, ids, *refs):
    packets = refs[:pieces]
    (coupling_1, gram_1, coupling_0, diag_0, off_0, off_1, cov_1, variances,
     full, diag) = refs[pieces:]
    n = full.shape[0]
    block = ids[1]
    start = ids[0]

    @pl.when(block < 2)
    def _():
        var_3 = unpack(full, diag, packets, start, paired)
        var_2 = diag[...]
        off_1[...] = (-mm(full[...], coupling_1[...])).astype(BF16)
        cov_1[...] = (gram_1[...] - mm_t(coupling_1[...], off_1[...])).astype(BF16)
        off_0[...] = (-mm(cov_1[...], coupling_0[...])).astype(BF16)
        for i in range(0, n, TILE):
            diag[:, i : i + TILE] = tile_diag(cov_1[i : i + TILE, i : i + TILE])
        product = coupling_0[...].astype(F32) * off_0[...].astype(F32)
        var_0 = diag_0[...] - jnp.sum(product, axis=0, keepdims=True)
        row = lax.broadcasted_iota(jnp.int32, variances.shape, 0)
        merged = jnp.where(row == 0, var_0, jnp.where(row == 1, diag[...], 0.0))
        merged = jnp.where(row == 2, var_2, jnp.where(row == 3, var_3, merged))
        variances[...] = merged.astype(BF16)


def last_kernel(ids, coupling_0, gram, off_0, off_1, cov_1, _, __, off_out, cov_out, cov, sems):
    rows = cov.shape[0]
    start = pl.multiple_of(ids[0], rows)
    block = ids[1]
    own = pl.ds(start, rows)

    @pl.when(block == 1)
    def _():
        one = pltpu.make_async_copy(off_1.at[own], off_out, sems.at[0])
        two = pltpu.make_async_copy(cov_1.at[own], cov_out, sems.at[1])
        one.start()
        two.start()
        one.wait()
        two.wait()

    @pl.when(block == 0)
    def _():
        one = pltpu.make_async_copy(off_0.at[own], off_out, sems.at[0])
        one.start()
        cov[...] = (gram[...] - mm_t(coupling_0[:, own], off_0[...])).astype(BF16)
        two = pltpu.make_async_copy(cov, cov_out, sems.at[1])
        two.start()
        one.wait()
        two.wait()


def deliver_kernel(ids, choice, mine, heard, out):
    block = ids[1]
    values = jnp.where(block < 2, mine[...].astype(F32), heard[...].astype(F32))
    for slot in range(SLOTS):
        line = jnp.zeros((1, out.shape[1]), F32)
        for t in range(TB):
            line += jnp.where(choice[slot * TB + t] == 1, values[t : t + 1], 0.0)
        out[slot : slot + 1, :] = line


def vmem(*arrays):
    return [pltpu.with_memory_space_constraint(a, pltpu.VMEM) for a in arrays]


def shards(linv, sub, owner):
    group = lax.axis_size("tm") // TB
    rows, n = linv.shape
    half = n // 2
    paired = group == 2
    dev = lax.axis_index("tm")
    member = dev % group
    block = dev // group
    ids = jnp.stack([member * rows, block]).astype(jnp.int32)

    def block_to_block(values, routes, members=range(group)):
        pairs = [(s * group + i, t * group + i) for s, t in routes for i in members]
        return lax.ppermute(values, "tm", pairs)

    def peer(piece, step=1):
        return lax.ppermute(piece, "tm", [(i, i ^ step) for i in range(TB * group)])

    def pieces_of(piece):
        if paired:
            return [piece, peer(piece)]
        step = 1
        while step < group:
            other = peer(piece, step)
            upper = (member // step) % 2 == 1
            piece = jnp.concatenate(
                [jnp.where(upper, other, piece), jnp.where(upper, piece, other)], 0
            )
            step *= 2
        return [piece]

    def packets_of(packet):
        return pieces_of(packet) if paired else pieces_of(packet[None])

    def after(values, *others):
        return lax.optimization_barrier((values, *others))[0]

    pieces = 2 if paired else 1
    packet_shape = (rows + SPARE, rows) if paired else (rows + SPARE, n)
    gathered = packet_shape if paired else (group, *packet_shape)
    whole = pltpu.VMEM((n, n), BF16)
    part = pltpu.VMEM((rows, n), BF16)
    hbm = jax.ShapeDtypeStruct((rows, n), BF16)
    square = pltpu.VMEM((n, n), BF16)

    factors = pieces_of(linv)
    lowers = pieces_of(sub)
    swap = [(1, 0), (0, 1)]
    heard_lower = block_to_block(sub, swap)

    coupling, packet, cov_3 = pl.pallas_call(
        functools.partial(first_kernel, pieces, paired),
        out_shape=(whole, pltpu.VMEM(packet_shape, BF16), part),
        in_specs=[SMEM] + [ANY] * (2 * pieces),
        out_specs=(VMEM, VMEM, VMEM),
        scratch_shapes=[
            square,
            square,
            pltpu.VMEM((rows, n), F32),
            pltpu.SemaphoreType.DMA((2, 2)),
        ],
        compiler_params=PARAMS,
        name="first",
    )(ids, *factors, *lowers)

    packet_2 = block_to_block(packet, [(3, 2)])
    late = after(linv, packet)
    heard_left = block_to_block(late[:, :half], swap)
    heard_right = block_to_block(late[:, half:], swap, range(group // 2, group))

    gram, off_rows, cov_rows = pl.pallas_call(
        functools.partial(gram_kernel, pieces),
        out_shape=(pltpu.VMEM((rows, n), F32), hbm, hbm),
        in_specs=[SMEM] + [ANY] * pieces + [VMEM, VMEM],
        out_specs=(VMEM, ANY, ANY),
        scratch_shapes=[
            square,
            pltpu.VMEM((rows, n), BF16),
            pltpu.SemaphoreType.DMA((1, 2)),
            pltpu.SemaphoreType.DMA((2,)),
        ],
        compiler_params=PARAMS,
        name="gram",
    )(ids, *factors, *vmem(coupling, cov_3))

    packet, off_2, cov_2 = pl.pallas_call(
        functools.partial(second_kernel, pieces, paired),
        out_shape=(pltpu.VMEM(packet_shape, BF16), whole, part),
        in_specs=[SMEM] + [VMEM] * (pieces + 2),
        out_specs=(VMEM, VMEM, VMEM),
        scratch_shapes=[square, pltpu.VMEM((1, n), F32)],
        compiler_params=PARAMS,
        name="second",
    )(ids, *vmem(*packets_of(packet_2), coupling, gram))

    packet_0 = block_to_block(packet, [(2, 0)])
    packet_1 = block_to_block(packet, [(2, 1)])

    heard_factor = jnp.concatenate([after(heard_left, packet), after(heard_right, packet)], 1)
    heard_factors = pieces_of(heard_factor)
    heard_lowers = pieces_of(after(heard_lower, packet))
    coupling_1, gram_1, coupling_0, diag_0, off_rows, cov_rows = pl.pallas_call(
        functools.partial(ready_kernel, pieces),
        out_shape=(
            whole,
            pltpu.VMEM((n, n), F32),
            whole,
            pltpu.VMEM((1, n), F32),
            hbm,
            hbm,
        ),
        in_specs=[SMEM] + [ANY] * (3 * pieces) + [VMEM] * 3 + [ANY, ANY],
        out_specs=(VMEM, VMEM, VMEM, VMEM, ANY, ANY),
        scratch_shapes=[
            square,
            square,
            square,
            pltpu.SemaphoreType.DMA((3, 2)),
            pltpu.SemaphoreType.DMA((2,)),
        ],
        input_output_aliases={3 * pieces + 4: 4, 3 * pieces + 5: 5},
        compiler_params=PARAMS,
        name="ready",
    )(
        ids,
        *factors,
        *heard_factors,
        *heard_lowers,
        *vmem(coupling, off_2, cov_2),
        off_rows,
        cov_rows,
    )

    carried = jnp.where(block == 0, packet_0, packet_1)
    off_0, off_1, cov_1, variances = pl.pallas_call(
        functools.partial(third_kernel, pieces, paired),
        out_shape=(whole, whole, whole, pltpu.VMEM((SPARE, n), BF16)),
        in_specs=[SMEM] + [VMEM] * (pieces + 4),
        out_specs=(VMEM, VMEM, VMEM, VMEM),
        scratch_shapes=[square, pltpu.VMEM((1, n), F32)],
        compiler_params=PARAMS,
        name="third",
    )(ids, *vmem(*packets_of(carried), coupling_1, gram_1, coupling_0, diag_0))

    heard = block_to_block(variances, [(0, 2), (1, 3)])

    off_rows, cov_rows = pl.pallas_call(
        last_kernel,
        out_shape=(hbm, hbm),
        in_specs=[SMEM] + [VMEM] * 5 + [ANY, ANY],
        out_specs=(ANY, ANY),
        scratch_shapes=[pltpu.VMEM((rows, n), BF16), pltpu.SemaphoreType.DMA((2,))],
        input_output_aliases={6: 0, 7: 1},
        compiler_params=PARAMS,
        name="last",
    )(ids, *vmem(coupling_0, gram, off_0, off_1, cov_1), off_rows, cov_rows)

    positions = lax.broadcasted_iota(jnp.int32, (TB, TB), 1)
    current = lax.broadcasted_iota(jnp.int32, (TB, TB), 0)
    same_owner = owner[:, None] == owner[None, :]
    slot_rank = jnp.sum(jnp.where(same_owner & (positions < current), 1, 0), axis=1)
    slot_iota = lax.broadcasted_iota(jnp.int32, (SLOTS, TB), 0)
    choice = (owner[None, :] == dev) & (slot_rank[None, :] == slot_iota)
    owned_var = pl.pallas_call(
        deliver_kernel,
        out_shape=jax.ShapeDtypeStruct((SLOTS, n), F32),
        in_specs=[SMEM, SMEM, VMEM, VMEM],
        out_specs=VMEM,
        compiler_params=PARAMS,
        name="deliver",
    )(ids, choice.astype(jnp.int32).reshape(SLOTS * TB), variances, heard)
    return (cov_rows, off_rows, owned_var)


def solution(mesh):
    return jax.shard_map(
        shards,
        mesh=mesh,
        in_specs=(P(("cfg", "tm"), None), P(("cfg", "tm"), None), P("cfg")),
        out_specs=(P(("cfg", "tm"), None), P(("cfg", "tm"), None), P(("cfg", "tm"), None)),
        check_vma=False,
    )
```

```python
import functools

import jax
import jax.numpy as jnp
from jax import lax
from jax.experimental import pallas as pl
from jax.experimental.pallas import tpu as pltpu
from jax.sharding import PartitionSpec as P


TB = 4
SLOTS = 2
SPARE = 16
TILE = 128

CONTRACT_FIRST = (((0,), (0,)), ((), ()))
BF16 = jnp.bfloat16
F32 = jnp.float32

HBM = pl.BlockSpec(memory_space=pltpu.HBM)
VMEM = pl.BlockSpec(memory_space=pltpu.VMEM)
SMEM = pl.BlockSpec(memory_space=pltpu.SMEM)
PARAMS = pltpu.CompilerParams(vmem_limit_bytes=36 << 20)


def mm(a, b):
    return jnp.dot(a, b, preferred_element_type=F32)


def mm_t(a, b):
    return lax.dot_general(a, b, CONTRACT_FIRST, preferred_element_type=F32)


def iotas(size):
    r = lax.broadcasted_iota(jnp.int32, (size, size), 0)
    c = lax.broadcasted_iota(jnp.int32, (size, size), 1)
    return r, c


def load_rows(target, pieces, start, sems):
    n = target.shape[0]
    if len(pieces) == 1:
        copies = [pltpu.make_async_copy(pieces[0], target, sems.at[0])]
    else:
        rows = pieces[0].shape[0]
        other = n - rows - start
        copies = [
            pltpu.make_async_copy(pieces[0], target.at[pl.ds(start, rows)], sems.at[0]),
            pltpu.make_async_copy(pieces[1], target.at[pl.ds(other, rows)], sems.at[1]),
        ]
    for copy in copies:
        copy.start()
    return copies


def couple(target, lower, factor):
    n = factor.shape[0]
    half = n // 2
    target[:, :half] = mm(lower[...], factor[:, :half]).astype(BF16)
    target[:, half:] = mm(lower[:, half:], factor[half:, half:]).astype(BF16)


def tile_diag(tile):
    r, c = iotas(TILE)
    return jnp.sum(jnp.where(r == c, tile.astype(F32), 0.0), axis=0, keepdims=True)


def pack(packet, cov, start, passenger, paired):
    rows, n = cov.shape
    row = lax.broadcasted_iota(jnp.int32, (SPARE, n if not paired else rows), 0)
    if not paired:
        packet[:rows, :] = cov[...]
        packet[rows:, :] = jnp.where(row == 0, passenger, 0.0).astype(BF16)
        return
    other = n - rows - start
    r, c = iotas(TILE)
    for i in range(0, rows, TILE):
        for j in range(0, rows, TILE):
            mine = cov[i : i + TILE, pl.ds(pl.multiple_of(start + j, TILE), TILE)]
            cross = cov[i : i + TILE, pl.ds(pl.multiple_of(other + j, TILE), TILE)]
            if j > i:
                tile = mine
            elif j < i:
                tile = cross
            else:
                tile = jnp.where(c >= r, mine.astype(F32), cross.astype(F32)).astype(BF16)
                dx = tile_diag(cross)
                spare = jnp.where(row[:, :TILE] == 0, dx, 0.0)
                for k in range(n // rows):
                    at = k * rows + i
                    spare = jnp.where(
                        row[:, :TILE] == k + 1, passenger[:, at : at + TILE], spare
                    )
                packet[rows:, i : i + TILE] = spare.astype(BF16)
            packet[i : i + TILE, j : j + TILE] = tile


def unpack(full, diag, packets, start, paired):
    n = full.shape[0]
    if not paired:
        (packet,) = packets
        rows = packet.shape[1] - SPARE
        for k in range(packet.shape[0]):
            full[k * rows : (k + 1) * rows, :] = packet[k, :rows, :]
        for i in range(0, n, TILE):
            diag[:, i : i + TILE] = tile_diag(full[i : i + TILE, i : i + TILE])
        return packet[0, rows:, :].astype(F32)[0:1]
    rows = packets[0].shape[0] - SPARE
    base = (start, n - rows - start)
    r, c = iotas(TILE)

    def put(at_row, i, at_col, j, tile):
        full[
            pl.ds(pl.multiple_of(at_row + i, TILE), TILE),
            pl.ds(pl.multiple_of(at_col + j, TILE), TILE),
        ] = tile

    spare = packets[0][rows:, :].astype(F32)
    for mine, yours in ((0, 1), (1, 0)):
        for i in range(0, rows, TILE):
            for j in range(0, rows, TILE):
                tile = packets[mine][i : i + TILE, j : j + TILE]
                flip = tile.T
                if j > i:
                    put(base[mine], i, base[mine], j, tile)
                    put(base[mine], j, base[mine], i, flip)
                elif j < i:
                    put(base[mine], i, base[yours], j, tile)
                    put(base[yours], j, base[mine], i, flip)
                else:
                    tile = tile.astype(F32)
                    flip = flip.astype(F32)
                    theirs = packets[yours][i : i + TILE, i : i + TILE].T.astype(F32)
                    own = jnp.where(c >= r, tile, flip)
                    put(base[mine], i, base[mine], i, own.astype(BF16))
                    dx = spare[0:1, i : i + TILE]
                    cross = jnp.where(c < r, tile, jnp.where(c > r, theirs, dx))
                    put(base[mine], i, base[yours], i, cross.astype(BF16))
                    diag[:, pl.ds(pl.multiple_of(base[mine] + i, TILE), TILE)] = tile_diag(own)
    return jnp.concatenate([spare[k + 1 : k + 2] for k in range(n // rows)], 1)


def fold_kernel(ids, factor, square, cross, sems):
    rows = factor.shape[0]
    half = rows // 2
    quarter = rows // 4
    start = pl.multiple_of(ids[0], rows)
    moves = [
        (factor.at[half:, pl.ds(start, rows)], square.at[:half]),
        (factor.at[:quarter, pl.ds(start, half)], square.at[half:, :half]),
        (factor.at[quarter:half, pl.ds(start, half)], square.at[half:, half:]),
        (factor.at[:, :rows], cross),
    ]
    copies = [pltpu.make_async_copy(s, t, sems.at[i]) for i, (s, t) in enumerate(moves)]
    for copy in copies:
        copy.start()
    for copy in copies:
        copy.wait()


def unfold(target, squares, crosses, start, sems):
    rows = squares[0].shape[0] * 4 // 3
    half = rows // 2
    quarter = rows // 4
    n = target.shape[0]
    moves = []
    for square, at in zip(squares, (start, n - rows - start)):
        moves += [
            (square.at[:half], target.at[pl.ds(at + half, half), pl.ds(at, rows)]),
            (square.at[half:, :half], target.at[pl.ds(at, quarter), pl.ds(at, half)]),
            (
                square.at[half:, half:],
                target.at[pl.ds(at + quarter, quarter), pl.ds(at, half)],
            ),
        ]
        zeros = jnp.zeros((half, half), BF16)
        target[pl.ds(at, half), pl.ds(pl.multiple_of(at + half, half), half)] = zeros
    target[:rows, rows:] = jnp.zeros((rows, n - rows), BF16)
    copies = [pltpu.make_async_copy(s, t, sems.at[i]) for i, (s, t) in enumerate(moves)]
    for copy in copies:
        copy.start()
    low = target.at[rows:, :rows]

    @pl.when(start == 0)
    def _():
        pltpu.make_async_copy(crosses[1], low, sems.at[len(moves)]).start()

    @pl.when(start != 0)
    def _():
        pltpu.make_async_copy(crosses[0], low, sems.at[len(moves)]).start()

    return copies + [pltpu.make_async_copy(crosses[0], low, sems.at[len(moves)])]


def first_kernel(pieces, paired, ids, *refs):
    factors, lowers = refs[:pieces], refs[pieces : 2 * pieces]
    coupling, packet, cov, factor, lower, total, sems = refs[2 * pieces :]
    rows = cov.shape[0]
    start = pl.multiple_of(ids[0], rows)
    block = ids[1]
    copies = load_rows(factor, factors, start, sems.at[0])
    copies += load_rows(lower, lowers, start, sems.at[1])
    for copy in copies:
        copy.wait()
    couple(coupling, lower, factor)

    @pl.when(block == TB - 1)
    def _():
        own = pl.ds(start, rows)
        total[...] = mm_t(factor[:, own], factor[...])
        cov[...] = (total[...] + mm_t(coupling[:, own], coupling[...])).astype(BF16)
        pack(packet, cov, start, jnp.zeros((1, factor.shape[1]), F32), paired)


def gram_kernel(pieces, ids, *refs):
    factors = refs[:pieces]
    coupling, cov, gram, off_out, cov_out, factor, off, sems, out_sems = refs[pieces:]
    rows = cov.shape[0]
    start = pl.multiple_of(ids[0], rows)
    block = ids[1]
    copies = load_rows(factor, factors, start, sems.at[0])
    for copy in copies:
        copy.wait()
    gram[...] = mm_t(factor[:, pl.ds(start, rows)], factor[...])

    @pl.when(block == TB - 1)
    def _():
        off[...] = -coupling[pl.ds(start, rows), :]
        one = pltpu.make_async_copy(off, off_out, out_sems.at[0])
        two = pltpu.make_async_copy(cov, cov_out, out_sems.at[1])
        one.start()
        two.start()
        one.wait()
        two.wait()


def heard_kernel(pieces, paired, ids, *refs):
    factors = refs[:pieces]
    parts = refs[pieces : len(refs) - 5]
    heard, gram_1, diag_0, factor, sems = refs[len(refs) - 5 :]
    rows = factors[0].shape[0] if paired else factor.shape[0]
    start = pl.multiple_of(ids[0], TILE)
    if paired:
        start = pl.multiple_of(ids[0], rows)
    block = ids[1]

    def finish(factor_1, factor_0):
        gram_1[...] = mm_t(factor_1[...], factor_1[...])
        diag_0[...] = jnp.sum(jnp.square(factor_0[...].astype(F32)), axis=0, keepdims=True)

    @pl.when(block < 2)
    def _():
        copies = load_rows(factor, factors, start, sems.at[0])
        if paired:
            copies += unfold(heard, parts[:2], parts[2:], start, sems.at[1])
        else:
            copies += load_rows(heard, parts, start, sems.at[1])
        for copy in copies:
            copy.wait()

        @pl.when(block == 0)
        def _():
            finish(heard, factor)

        @pl.when(block == 1)
        def _():
            finish(factor, heard)


def second_kernel(pieces, paired, ids, *refs):
    packets = refs[:pieces]
    coupling, gram, packet, off, cov, full, diag = refs[pieces:]
    rows = cov.shape[0]
    start = pl.multiple_of(ids[0], rows)
    block = ids[1]

    @pl.when(block == TB - 2)
    def _():
        unpack(full, diag, packets, start, paired)
        off[...] = (-mm(full[...], coupling[...])).astype(BF16)
        cov[...] = (gram[...] - mm_t(coupling[:, pl.ds(start, rows)], off[...])).astype(BF16)
        pack(packet, cov, start, diag[...], paired)


def ready_kernel(pieces, ids, *refs):
    lowers = refs[:pieces]
    (heard, coupling, off, cov, _, _, coupling_1, coupling_0, off_out, cov_out,
     lower, sems, out_sems) = refs[pieces:]
    rows = cov.shape[0]
    start = pl.multiple_of(ids[0], rows)
    block = ids[1]

    @pl.when(block == TB - 2)
    def _():
        one = pltpu.make_async_copy(off.at[pl.ds(start, rows)], off_out, out_sems.at[0])
        two = pltpu.make_async_copy(cov, cov_out, out_sems.at[1])
        one.start()
        two.start()
        one.wait()
        two.wait()

    @pl.when(block < 2)
    def _():
        copies = load_rows(lower, lowers, start, sems.at[0])

        @pl.when(block == 0)
        def _():
            coupling_0[...] = coupling[...]

        @pl.when(block == 1)
        def _():
            coupling_1[...] = coupling[...]

        for copy in copies:
            copy.wait()

        @pl.when(block == 0)
        def _():
            couple(coupling_1, lower, heard)

        @pl.when(block == 1)
        def _():
            couple(coupling_0, lower, heard)


def merge_kernel(ids, at_0, at_1, out, sem):
    block = ids[1]

    @pl.when(block == 0)
    def _():
        copy = pltpu.make_async_copy(at_0, out, sem.at[0])
        copy.start()
        copy.wait()

    @pl.when(block == 1)
    def _():
        copy = pltpu.make_async_copy(at_1, out, sem.at[0])
        copy.start()
        copy.wait()


def third_kernel(pieces, paired, ids, *refs):
    packets = refs[:pieces]
    (coupling_1, gram_1, coupling_0, diag_0, off_0, off_1, cov_1, variances,
     full, diag) = refs[pieces:]
    n = full.shape[0]
    start = ids[0]
    block = ids[1]

    @pl.when(block < 2)
    def _():
        var_3 = unpack(full, diag, packets, start, paired)
        var_2 = diag[...]
        off_1[...] = (-mm(full[...], coupling_1[...])).astype(BF16)
        cov_1[...] = (gram_1[...] - mm_t(coupling_1[...], off_1[...])).astype(BF16)
        off_0[...] = (-mm(cov_1[...], coupling_0[...])).astype(BF16)
        for i in range(0, n, TILE):
            diag[:, i : i + TILE] = tile_diag(cov_1[i : i + TILE, i : i + TILE])
        product = coupling_0[...].astype(F32) * off_0[...].astype(F32)
        var_0 = diag_0[...] - jnp.sum(product, axis=0, keepdims=True)
        row = lax.broadcasted_iota(jnp.int32, variances.shape, 0)
        merged = jnp.where(row == 0, var_0, jnp.where(row == 1, diag[...], 0.0))
        merged = jnp.where(row == 2, var_2, jnp.where(row == 3, var_3, merged))
        variances[...] = merged.astype(BF16)


def last_kernel(ids, coupling_0, gram, off_0, off_1, cov_1, _, __, off_out, cov_out, cov, sems):
    rows = cov.shape[0]
    start = pl.multiple_of(ids[0], rows)
    block = ids[1]
    own = pl.ds(start, rows)

    @pl.when(block == 1)
    def _():
        one = pltpu.make_async_copy(off_1.at[own], off_out, sems.at[0])
        two = pltpu.make_async_copy(cov_1.at[own], cov_out, sems.at[1])
        one.start()
        two.start()
        one.wait()
        two.wait()

    @pl.when(block == 0)
    def _():
        one = pltpu.make_async_copy(off_0.at[own], off_out, sems.at[0])
        one.start()
        cov[...] = (gram[...] - mm_t(coupling_0[:, own], off_0[...])).astype(BF16)
        two = pltpu.make_async_copy(cov, cov_out, sems.at[1])
        two.start()
        one.wait()
        two.wait()


def deliver_kernel(ids, owner, mine, heard, out):
    block = ids[1]
    dev = ids[2]
    values = jnp.where(block < 2, mine[...].astype(F32), heard[...].astype(F32))
    lines = [jnp.zeros((1, out.shape[1]), F32) for _ in range(SLOTS)]
    for t in range(TB):
        rank = jnp.int32(0)
        for before in range(t):
            rank += (owner[before] == owner[t]).astype(jnp.int32)
        for slot in range(SLOTS):
            here = jnp.logical_and(owner[t] == dev, rank == slot)
            lines[slot] += jnp.where(here, values[t : t + 1], 0.0)
    for slot in range(SLOTS):
        out[slot : slot + 1, :] = lines[slot]


def shards(linv, sub, owner):
    group = lax.axis_size("tm") // TB
    rows, n = linv.shape
    paired = group == 2
    dev = lax.axis_index("tm")
    member = dev % group
    block = dev // group
    ids = jnp.stack([member * rows, block, dev]).astype(jnp.int32)

    def block_to_block(values, routes, members=range(group)):
        pairs = [(s * group + i, t * group + i) for s, t in routes for i in members]
        return lax.ppermute(values, "tm", pairs)

    def peer(piece, step=1):
        return lax.ppermute(piece, "tm", [(i, i ^ step) for i in range(TB * group)])

    def pieces_of(piece):
        if paired:
            return [piece, peer(piece)]
        step = 1
        while step < group:
            other = peer(piece, step)
            upper = (member // step) % 2 == 1
            piece = jnp.concatenate(
                [jnp.where(upper, other, piece), jnp.where(upper, piece, other)], 0
            )
            step *= 2
        return [piece]

    def packets_of(packet):
        return pieces_of(packet) if paired else pieces_of(packet[None])

    def after(values, *others):
        return lax.optimization_barrier((values, *others))[0]

    def call(kernel, out, inputs, spaces, scratch, aliases=None):
        shapes = tuple(
            pltpu.HBM(o[1], o[2]) if o[0] is HBM else pltpu.VMEM(o[1], o[2]) for o in out
        )
        placed = [
            x if space is SMEM else pltpu.with_memory_space_constraint(x, space.memory_space)
            for x, space in zip(inputs, spaces, strict=True)
        ]
        return pl.pallas_call(
            kernel,
            out_shape=shapes,
            in_specs=list(spaces),
            out_specs=tuple(o[0] for o in out),
            scratch_shapes=scratch,
            input_output_aliases=aliases or {},
            compiler_params=PARAMS,
        )(*placed)

    def sems(*shape):
        return pltpu.SemaphoreType.DMA(shape)

    pieces = 2 if paired else 1
    packet_shape = (rows + SPARE, rows) if paired else (rows + SPARE, n)
    whole = (VMEM, (n, n), BF16)
    part = (VMEM, (rows, n), BF16)
    out_rows = (HBM, (rows, n), BF16)
    square = pltpu.VMEM((n, n), BF16)

    factors = pieces_of(linv)
    lowers = pieces_of(sub)
    swap = [(1, 0), (0, 1)]
    if paired:
        folded, cross = call(
            fold_kernel,
            [(HBM, (rows * 3 // 4, rows), BF16), (HBM, (rows, rows), BF16)],
            [ids, linv],
            [SMEM, HBM],
            [sems(4)],
        )
        raw = [block_to_block(folded, swap), block_to_block(cross, swap, range(1, 2))]
    else:
        raw = [block_to_block(linv, swap)]
    raw_lower = block_to_block(sub, swap)

    coupling, packet, cov_3 = call(
        functools.partial(first_kernel, pieces, paired),
        [whole, (VMEM, packet_shape, BF16), part],
        [ids, *factors, *lowers],
        [SMEM] + [HBM] * (2 * pieces),
        [square, square, pltpu.VMEM((rows, n), F32), sems(2, 2)],
    )
    packet_2 = block_to_block(packet, [(3, 2)])

    gram, off_rows, cov_rows = call(
        functools.partial(gram_kernel, pieces),
        [(VMEM, (rows, n), F32), out_rows, out_rows],
        [ids, *factors, coupling, cov_3],
        [SMEM] + [HBM] * pieces + [VMEM, VMEM],
        [square, pltpu.VMEM((rows, n), BF16), sems(1, 2), sems(2)],
    )
    parts = [x for piece in raw for x in pieces_of(after(piece, gram))]
    heard_factor, gram_1, diag_0 = call(
        functools.partial(heard_kernel, pieces, paired),
        [whole, (VMEM, (n, n), F32), (VMEM, (1, n), F32)],
        [ids, *factors, *parts],
        [SMEM] + [HBM] * (pieces + len(parts)),
        [square, sems(2, 8)],
    )

    packet, off_2, cov_2 = call(
        functools.partial(second_kernel, pieces, paired),
        [(VMEM, packet_shape, BF16), whole, part],
        [ids, *packets_of(packet_2), coupling, gram],
        [SMEM] + [VMEM] * (pieces + 2),
        [square, pltpu.VMEM((1, n), F32)],
    )
    packet_0 = block_to_block(packet, [(2, 0)])
    packet_1 = block_to_block(packet, [(2, 1)])

    raw_lowers = pieces_of(after(raw_lower, packet))
    coupling_1, coupling_0, off_rows, cov_rows = call(
        functools.partial(ready_kernel, pieces),
        [whole, whole, out_rows, out_rows],
        [ids, *raw_lowers, heard_factor, coupling, off_2, cov_2, off_rows, cov_rows],
        [SMEM] + [HBM] * pieces + [VMEM] * 4 + [HBM, HBM],
        [square, sems(1, 2), sems(2)],
        {pieces + 5: 2, pieces + 6: 3},
    )

    (carried,) = call(
        merge_kernel,
        [(VMEM, packet_shape, BF16)],
        [ids, packet_0, packet_1],
        [SMEM, VMEM, VMEM],
        [sems(1)],
    )
    off_0, off_1, cov_1, variances = call(
        functools.partial(third_kernel, pieces, paired),
        [whole, whole, whole, (VMEM, (SPARE, n), BF16)],
        [ids, *packets_of(carried), coupling_1, gram_1, coupling_0, diag_0],
        [SMEM] + [VMEM] * (pieces + 4),
        [square, pltpu.VMEM((1, n), F32)],
    )
    heard = block_to_block(variances, [(0, 2), (1, 3)])

    off_rows, cov_rows = call(
        last_kernel,
        [out_rows, out_rows],
        [ids, coupling_0, gram, off_0, off_1, cov_1, off_rows, cov_rows],
        [SMEM] + [VMEM] * 5 + [HBM, HBM],
        [pltpu.VMEM((rows, n), BF16), sems(2)],
        {6: 0, 7: 1},
    )
    (owned_var,) = call(
        deliver_kernel,
        [(VMEM, (SLOTS, n), F32)],
        [ids, owner, variances, heard],
        [SMEM, SMEM, VMEM, VMEM],
        [],
    )
    return (cov_rows, off_rows, owned_var)


def solution(mesh):
    return jax.shard_map(
        shards,
        mesh=mesh,
        in_specs=(P(("cfg", "tm"), None), P(("cfg", "tm"), None), P("cfg")),
        out_specs=(P(("cfg", "tm"), None), P(("cfg", "tm"), None), P(("cfg", "tm"), None)),
        check_vma=False,
    )
```

```python
import functools

import jax
import jax.numpy as jnp
from jax import lax
from jax.experimental import pallas as pl
from jax.experimental.pallas import tpu as pltpu
from jax.sharding import PartitionSpec as P


TB = 4
SLOTS = 2
SPARE = 16
TILE = 128

CONTRACT_FIRST = (((0,), (0,)), ((), ()))
BF16 = jnp.bfloat16
F32 = jnp.float32

HBM = pl.BlockSpec(memory_space=pltpu.HBM)
VMEM = pl.BlockSpec(memory_space=pltpu.VMEM)
SMEM = pl.BlockSpec(memory_space=pltpu.SMEM)
PARAMS = pltpu.CompilerParams(vmem_limit_bytes=36 << 20)


def mm(a, b):
    return jnp.dot(a, b, preferred_element_type=F32)


def mm_t(a, b):
    return lax.dot_general(a, b, CONTRACT_FIRST, preferred_element_type=F32)


def iotas(size):
    r = lax.broadcasted_iota(jnp.int32, (size, size), 0)
    c = lax.broadcasted_iota(jnp.int32, (size, size), 1)
    return r, c


def couple(target, lowers, factor, start):
    n = factor.shape[0]
    half = n // 2
    rows = lowers[0].shape[0]
    for lower, at in zip(lowers, (start if rows < n else 0, n - rows - start)):
        here = pl.ds(pl.multiple_of(at, rows), rows)
        target[here, :half] = mm(lower[...], factor[:, :half]).astype(BF16)
        target[here, half:] = mm(lower[:, half:], factor[half:, half:]).astype(BF16)


def write_out(values, outs, sems):
    copies = [
        pltpu.make_async_copy(v, o, sems.at[i]) for i, (v, o) in enumerate(zip(values, outs))
    ]
    for copy in copies:
        copy.start()
    for copy in copies:
        copy.wait()


def tile_diag(tile):
    r, c = iotas(TILE)
    return jnp.sum(jnp.where(r == c, tile.astype(F32), 0.0), axis=0, keepdims=True)


def pack(packet, cov, start, passenger, paired):
    rows, n = cov.shape
    row = lax.broadcasted_iota(jnp.int32, (SPARE, n if not paired else rows), 0)
    if not paired:
        packet[:rows, :] = cov[...]
        packet[rows:, :] = jnp.where(row == 0, passenger, 0.0).astype(BF16)
        return
    other = n - rows - start
    r, c = iotas(TILE)
    for i in range(0, rows, TILE):
        for j in range(0, rows, TILE):
            mine = cov[i : i + TILE, pl.ds(pl.multiple_of(start + j, TILE), TILE)]
            cross = cov[i : i + TILE, pl.ds(pl.multiple_of(other + j, TILE), TILE)]
            if j > i:
                tile = mine
            elif j < i:
                tile = cross
            else:
                tile = jnp.where(c >= r, mine.astype(F32), cross.astype(F32)).astype(BF16)
                dx = tile_diag(cross)
                spare = jnp.where(row[:, :TILE] == 0, dx, 0.0)
                for k in range(n // rows):
                    at = k * rows + i
                    spare = jnp.where(
                        row[:, :TILE] == k + 1, passenger[:, at : at + TILE], spare
                    )
                packet[rows:, i : i + TILE] = spare.astype(BF16)
            packet[i : i + TILE, j : j + TILE] = tile


def unpack(full, diag, packets, start, paired):
    n = full.shape[0]
    if not paired:
        (packet,) = packets
        rows = packet.shape[1] - SPARE
        for k in range(packet.shape[0]):
            full[k * rows : (k + 1) * rows, :] = packet[k, :rows, :]
        for i in range(0, n, TILE):
            diag[:, i : i + TILE] = tile_diag(full[i : i + TILE, i : i + TILE])
        return packet[0, rows:, :].astype(F32)[0:1]
    rows = packets[0].shape[0] - SPARE
    base = (start, n - rows - start)
    r, c = iotas(TILE)

    def put(at_row, i, at_col, j, tile):
        full[
            pl.ds(pl.multiple_of(at_row + i, TILE), TILE),
            pl.ds(pl.multiple_of(at_col + j, TILE), TILE),
        ] = tile

    spare = packets[0][rows:, :].astype(F32)
    for mine, yours in ((0, 1), (1, 0)):
        for i in range(0, rows, TILE):
            for j in range(0, rows, TILE):
                tile = packets[mine][i : i + TILE, j : j + TILE]
                flip = tile.T
                if j > i:
                    put(base[mine], i, base[mine], j, tile)
                    put(base[mine], j, base[mine], i, flip)
                elif j < i:
                    put(base[mine], i, base[yours], j, tile)
                    put(base[yours], j, base[mine], i, flip)
                else:
                    tile = tile.astype(F32)
                    flip = flip.astype(F32)
                    theirs = packets[yours][i : i + TILE, i : i + TILE].T.astype(F32)
                    own = jnp.where(c >= r, tile, flip)
                    put(base[mine], i, base[mine], i, own.astype(BF16))
                    dx = spare[0:1, i : i + TILE]
                    cross = jnp.where(c < r, tile, jnp.where(c > r, theirs, dx))
                    put(base[mine], i, base[yours], i, cross.astype(BF16))
                    diag[:, pl.ds(pl.multiple_of(base[mine] + i, TILE), TILE)] = tile_diag(own)
    return jnp.concatenate([spare[k + 1 : k + 2] for k in range(n // rows)], 1)


def fold_kernel(ids, factor, square, cross, sems):
    rows = factor.shape[0]
    half = rows // 2
    quarter = rows // 4
    start = pl.multiple_of(ids[0], rows)
    moves = [
        (factor.at[half:, pl.ds(start, rows)], square.at[:half]),
        (factor.at[:quarter, pl.ds(start, half)], square.at[half:, :half]),
        (factor.at[quarter:half, pl.ds(start, half)], square.at[half:, half:]),
        (factor.at[:, :rows], cross),
    ]
    copies = [pltpu.make_async_copy(s, t, sems.at[i]) for i, (s, t) in enumerate(moves)]
    for copy in copies:
        copy.start()
    for copy in copies:
        copy.wait()


def unfold(target, squares, crosses, start, sems):
    rows = squares[0].shape[0] * 4 // 3
    half = rows // 2
    quarter = rows // 4
    n = target.shape[0]
    moves = []
    for square, at in zip(squares, (start, n - rows - start)):
        moves += [
            (square.at[:half], target.at[pl.ds(at + half, half), pl.ds(at, rows)]),
            (square.at[half:, :half], target.at[pl.ds(at, quarter), pl.ds(at, half)]),
            (
                square.at[half:, half:],
                target.at[pl.ds(at + quarter, quarter), pl.ds(at, half)],
            ),
        ]
        zeros = jnp.zeros((half, half), BF16)
        target[pl.ds(at, half), pl.ds(pl.multiple_of(at + half, half), half)] = zeros
    target[:rows, rows:] = jnp.zeros((rows, n - rows), BF16)
    copies = [pltpu.make_async_copy(s, t, sems.at[i]) for i, (s, t) in enumerate(moves)]
    for copy in copies:
        copy.start()
    low = target.at[rows:, :rows]

    @pl.when(start == 0)
    def _():
        pltpu.make_async_copy(crosses[1], low, sems.at[len(moves)]).start()

    @pl.when(start != 0)
    def _():
        pltpu.make_async_copy(crosses[0], low, sems.at[len(moves)]).start()

    return copies + [pltpu.make_async_copy(crosses[0], low, sems.at[len(moves)])]


def place(target, pieces, start):
    n = target.shape[0]
    if len(pieces) == 1:
        target[...] = pieces[0][...]
        return
    rows = pieces[0].shape[0]
    for piece, at in zip(pieces, (start, n - rows - start)):
        target[pl.ds(pl.multiple_of(at, rows), rows), :] = piece[...]


def gram_kernel(pieces, ids, *refs):
    pieces, (factor, gram) = refs[:pieces], refs[pieces:]
    rows, n = gram.shape
    half = n // 2
    start = pl.multiple_of(ids[0], rows)
    own = pl.ds(start, rows)
    place(factor, pieces, start)
    gram[:, :half] = mm_t(factor[:, own], factor[:, :half])
    gram[:, half:] = mm_t(factor[half:, own], factor[half:, half:])


def first_kernel(pieces, paired, ids, *refs):
    lowers = refs[:pieces]
    factor, gram, coupling, packet, cov = refs[pieces:]
    rows, n = cov.shape
    start = pl.multiple_of(ids[0], rows)
    block = ids[1]
    couple(coupling, lowers, factor, start)

    @pl.when(block == TB - 1)
    def _():
        own = pl.ds(start, rows)
        cov[...] = (gram[...] + mm_t(coupling[:, own], coupling[...])).astype(BF16)
        pack(packet, cov, start, jnp.zeros((1, n), F32), paired)


def heard_kernel(parts, paired, ids, *refs):
    parts, rest = refs[:parts], refs[parts:]
    (factor, coupling, cov, heard, gram_1, diag_0, off_out, cov_out,
     off, sems, out_sems) = rest
    rows = cov.shape[0]
    start = pl.multiple_of(ids[0], rows)
    block = ids[1]

    def finish(factor_1, factor_0):
        gram_1[...] = mm_t(factor_1[...], factor_1[...])
        diag_0[...] = jnp.sum(jnp.square(factor_0[...].astype(F32)), axis=0, keepdims=True)

    @pl.when(block == TB - 1)
    def _():
        off[...] = -coupling[pl.ds(start, rows), :]
        write_out((off, cov), (off_out, cov_out), out_sems)

    @pl.when(block < 2)
    def _():
        if paired:
            for copy in unfold(heard, parts[:2], parts[2:], start, sems):
                copy.wait()
        else:
            place(heard, parts, start)

        @pl.when(block == 0)
        def _():
            finish(heard, factor)

        @pl.when(block == 1)
        def _():
            finish(factor, heard)


def second_kernel(pieces, paired, ids, *refs):
    packets = refs[:pieces]
    coupling, gram, packet, off, cov, full, diag = refs[pieces:]
    rows = cov.shape[0]
    start = pl.multiple_of(ids[0], rows)
    block = ids[1]

    @pl.when(block == TB - 2)
    def _():
        unpack(full, diag, packets, start, paired)
        off[...] = (-mm(full[...], coupling[...])).astype(BF16)
        cov[...] = (gram[...] - mm_t(coupling[:, pl.ds(start, rows)], off[...])).astype(BF16)
        pack(packet, cov, start, diag[...], paired)


def ready_kernel(pieces, ids, *refs):
    lowers = refs[:pieces]
    (heard, coupling, off, cov, _, _, coupling_1, coupling_0, off_out, cov_out,
     out_sems) = refs[pieces:]
    rows = cov.shape[0]
    start = pl.multiple_of(ids[0], rows)
    block = ids[1]

    @pl.when(block == TB - 2)
    def _():
        write_out((off.at[pl.ds(start, rows)], cov), (off_out, cov_out), out_sems)

    @pl.when(block == 0)
    def _():
        coupling_0[...] = coupling[...]
        couple(coupling_1, lowers, heard, start)

    @pl.when(block == 1)
    def _():
        coupling_1[...] = coupling[...]
        couple(coupling_0, lowers, heard, start)


def merge_kernel(ids, at_0, at_1, out, sem):
    block = ids[1]

    @pl.when(block == 0)
    def _():
        copy = pltpu.make_async_copy(at_0, out, sem.at[0])
        copy.start()
        copy.wait()

    @pl.when(block == 1)
    def _():
        copy = pltpu.make_async_copy(at_1, out, sem.at[0])
        copy.start()
        copy.wait()


def third_kernel(pieces, paired, ids, *refs):
    packets = refs[:pieces]
    (coupling_1, gram_1, coupling_0, diag_0, off_0, off_1, cov_1, variances,
     full, diag) = refs[pieces:]
    n = full.shape[0]
    start = ids[0]
    block = ids[1]

    @pl.when(block < 2)
    def _():
        var_3 = unpack(full, diag, packets, start, paired)
        var_2 = diag[...]
        off_1[...] = (-mm(full[...], coupling_1[...])).astype(BF16)
        cov_1[...] = (gram_1[...] - mm_t(coupling_1[...], off_1[...])).astype(BF16)
        off_0[...] = (-mm(cov_1[...], coupling_0[...])).astype(BF16)
        for i in range(0, n, TILE):
            diag[:, i : i + TILE] = tile_diag(cov_1[i : i + TILE, i : i + TILE])
        product = coupling_0[...].astype(F32) * off_0[...].astype(F32)
        var_0 = diag_0[...] - jnp.sum(product, axis=0, keepdims=True)
        row = lax.broadcasted_iota(jnp.int32, variances.shape, 0)
        merged = jnp.where(row == 0, var_0, jnp.where(row == 1, diag[...], 0.0))
        merged = jnp.where(row == 2, var_2, jnp.where(row == 3, var_3, merged))
        variances[...] = merged.astype(BF16)


def last_kernel(ids, coupling_0, gram, off_0, off_1, cov_1, _, __, off_out, cov_out, cov, sems):
    rows = cov.shape[0]
    start = pl.multiple_of(ids[0], rows)
    block = ids[1]
    own = pl.ds(start, rows)

    @pl.when(block == 1)
    def _():
        one = pltpu.make_async_copy(off_1.at[own], off_out, sems.at[0])
        two = pltpu.make_async_copy(cov_1.at[own], cov_out, sems.at[1])
        one.start()
        two.start()
        one.wait()
        two.wait()

    @pl.when(block == 0)
    def _():
        one = pltpu.make_async_copy(off_0.at[own], off_out, sems.at[0])
        one.start()
        cov[...] = (gram[...] - mm_t(coupling_0[:, own], off_0[...])).astype(BF16)
        two = pltpu.make_async_copy(cov, cov_out, sems.at[1])
        two.start()
        one.wait()
        two.wait()


def deliver_kernel(ids, owner, mine, heard, out):
    block = ids[1]
    dev = ids[2]
    values = jnp.where(block < 2, mine[...].astype(F32), heard[...].astype(F32))
    lines = [jnp.zeros((1, out.shape[1]), F32) for _ in range(SLOTS)]
    for t in range(TB):
        rank = jnp.int32(0)
        for before in range(t):
            rank += (owner[before] == owner[t]).astype(jnp.int32)
        for slot in range(SLOTS):
            here = jnp.logical_and(owner[t] == dev, rank == slot)
            lines[slot] += jnp.where(here, values[t : t + 1], 0.0)
    for slot in range(SLOTS):
        out[slot : slot + 1, :] = lines[slot]


def shards(linv, sub, owner):
    group = lax.axis_size("tm") // TB
    rows, n = linv.shape
    paired = group == 2
    dev = lax.axis_index("tm")
    member = dev % group
    block = dev // group
    ids = jnp.stack([member * rows, block, dev]).astype(jnp.int32)

    def block_to_block(values, routes, members=range(group)):
        pairs = [(s * group + i, t * group + i) for s, t in routes for i in members]
        return lax.ppermute(values, "tm", pairs)

    def peer(piece, step=1):
        return lax.ppermute(piece, "tm", [(i, i ^ step) for i in range(TB * group)])

    def pieces_of(piece):
        if paired:
            return [piece, peer(piece)]
        step = 1
        while step < group:
            other = peer(piece, step)
            upper = (member // step) % 2 == 1
            piece = jnp.concatenate(
                [jnp.where(upper, other, piece), jnp.where(upper, piece, other)], 0
            )
            step *= 2
        return [piece]

    def packets_of(packet):
        return pieces_of(packet) if paired else pieces_of(packet[None])

    def after(values, *others):
        return lax.optimization_barrier((values, *others))[0]

    def call(kernel, out, inputs, spaces, scratch, aliases=None):
        shapes = tuple(
            pltpu.HBM(o[1], o[2]) if o[0] is HBM else pltpu.VMEM(o[1], o[2]) for o in out
        )
        placed = [
            x if space is SMEM else pltpu.with_memory_space_constraint(x, space.memory_space)
            for x, space in zip(inputs, spaces, strict=True)
        ]
        return pl.pallas_call(
            kernel,
            out_shape=shapes,
            in_specs=list(spaces),
            out_specs=tuple(o[0] for o in out),
            scratch_shapes=scratch,
            input_output_aliases=aliases or {},
            compiler_params=PARAMS,
        )(*placed)

    def sems(*shape):
        return pltpu.SemaphoreType.DMA(shape)

    pieces = 2 if paired else 1
    packet_shape = (rows + SPARE, rows) if paired else (rows + SPARE, n)
    whole = (VMEM, (n, n), BF16)
    part = (VMEM, (rows, n), BF16)
    out_rows = (HBM, (rows, n), BF16)
    square = pltpu.VMEM((n, n), BF16)

    factors = pieces_of(linv)
    lowers = pieces_of(sub)
    swap = [(1, 0), (0, 1)]
    if paired:
        folded, cross = call(
            fold_kernel,
            [(VMEM, (rows * 3 // 4, rows), BF16), (VMEM, (rows, rows), BF16)],
            [ids, linv],
            [SMEM, HBM],
            [sems(4)],
        )
        raw = [block_to_block(folded, swap), block_to_block(cross, swap, range(1, 2))]
    else:
        raw = [block_to_block(linv, swap)]
    raw_lower = block_to_block(sub, swap)

    factor, gram = call(
        functools.partial(gram_kernel, pieces),
        [whole, (VMEM, (rows, n), F32)],
        [ids, *factors],
        [SMEM] + [VMEM] * pieces,
        [],
    )
    coupling, packet, cov_3 = call(
        functools.partial(first_kernel, pieces, paired),
        [whole, (VMEM, packet_shape, BF16), part],
        [ids, *lowers, factor, gram],
        [SMEM] + [VMEM] * (pieces + 2),
        [],
    )
    packet_2 = block_to_block(packet, [(3, 2)])

    parts = [x for piece in raw for x in pieces_of(after(piece, packet))]
    heard_factor, gram_1, diag_0, off_rows, cov_rows = call(
        functools.partial(heard_kernel, len(parts), paired),
        [whole, (VMEM, (n, n), F32), (VMEM, (1, n), F32), out_rows, out_rows],
        [ids, *parts, factor, coupling, cov_3],
        [SMEM] + [VMEM] * (len(parts) + 3),
        [pltpu.VMEM((rows, n), BF16), sems(8), sems(2)],
    )

    packet, off_2, cov_2 = call(
        functools.partial(second_kernel, pieces, paired),
        [(VMEM, packet_shape, BF16), whole, part],
        [ids, *packets_of(packet_2), coupling, gram],
        [SMEM] + [VMEM] * (pieces + 2),
        [square, pltpu.VMEM((1, n), F32)],
    )
    packet_0 = block_to_block(packet, [(2, 0)])
    packet_1 = block_to_block(packet, [(2, 1)])

    raw_lowers = pieces_of(after(raw_lower, packet))
    coupling_1, coupling_0, off_rows, cov_rows = call(
        functools.partial(ready_kernel, pieces),
        [whole, whole, out_rows, out_rows],
        [ids, *raw_lowers, heard_factor, coupling, off_2, cov_2, off_rows, cov_rows],
        [SMEM] + [VMEM] * (pieces + 4) + [HBM, HBM],
        [sems(2)],
        {pieces + 5: 2, pieces + 6: 3},
    )

    (carried,) = call(
        merge_kernel,
        [(VMEM, packet_shape, BF16)],
        [ids, packet_0, packet_1],
        [SMEM, VMEM, VMEM],
        [sems(1)],
    )
    off_0, off_1, cov_1, variances = call(
        functools.partial(third_kernel, pieces, paired),
        [whole, whole, whole, (VMEM, (SPARE, n), BF16)],
        [ids, *packets_of(carried), coupling_1, gram_1, coupling_0, diag_0],
        [SMEM] + [VMEM] * (pieces + 4),
        [square, pltpu.VMEM((1, n), F32)],
    )
    heard = block_to_block(variances, [(0, 2), (1, 3)])

    off_rows, cov_rows = call(
        last_kernel,
        [out_rows, out_rows],
        [ids, coupling_0, gram, off_0, off_1, cov_1, off_rows, cov_rows],
        [SMEM] + [VMEM] * 5 + [HBM, HBM],
        [pltpu.VMEM((rows, n), BF16), sems(2)],
        {6: 0, 7: 1},
    )
    (owned_var,) = call(
        deliver_kernel,
        [(VMEM, (SLOTS, n), F32)],
        [ids, owner, variances, heard],
        [SMEM, SMEM, VMEM, VMEM],
        [],
    )
    return (cov_rows, off_rows, owned_var)


def solution(mesh):
    return jax.shard_map(
        shards,
        mesh=mesh,
        in_specs=(P(("cfg", "tm"), None), P(("cfg", "tm"), None), P("cfg")),
        out_specs=(P(("cfg", "tm"), None), P(("cfg", "tm"), None), P(("cfg", "tm"), None)),
        check_vma=False,
    )
```

```python
import functools

import jax
import jax.numpy as jnp
from jax import lax
from jax.experimental import pallas as pl
from jax.experimental.pallas import tpu as pltpu
from jax.sharding import PartitionSpec as P


TB = 4
SLOTS = 2
SPARE = 16
TILE = 128

CONTRACT_FIRST = (((0,), (0,)), ((), ()))
BF16 = jnp.bfloat16
F32 = jnp.float32

HBM = pl.BlockSpec(memory_space=pltpu.HBM)
VMEM = pl.BlockSpec(memory_space=pltpu.VMEM)
SMEM = pl.BlockSpec(memory_space=pltpu.SMEM)
PARAMS = pltpu.CompilerParams(vmem_limit_bytes=18 << 20)


def located(kernel, rows, group):
    def body(*refs):
        dev = lax.axis_index("tm")
        member = lax.rem(dev, jnp.int32(group))
        kernel((member * rows, lax.div(dev, jnp.int32(group)), dev), *refs)

    return body


def mm(a, b):
    return jnp.dot(a, b, preferred_element_type=F32)


def mm_t(a, b):
    return lax.dot_general(a, b, CONTRACT_FIRST, preferred_element_type=F32)


def iotas(size):
    r = lax.broadcasted_iota(jnp.int32, (size, size), 0)
    c = lax.broadcasted_iota(jnp.int32, (size, size), 1)
    return r, c


def couple(target, lowers, factor):
    half = factor.shape[0] // 2
    for lower, at in lowers:
        here = pl.ds(at, lower.shape[0])
        target[here, :half] = mm(lower[...], factor[:, :half]).astype(BF16)
        target[here, half:] = mm(lower[:, half:], factor[half:, half:]).astype(BF16)


def write_out(values, outs, sems):
    copies = [
        pltpu.make_async_copy(v, o, sems.at[i]) for i, (v, o) in enumerate(zip(values, outs))
    ]
    for copy in copies:
        copy.start()
    for copy in copies:
        copy.wait()


def tile_diag(tile):
    r, c = iotas(TILE)
    return jnp.sum(jnp.where(r == c, tile.astype(F32), 0.0), axis=0, keepdims=True)


def pack(packet, cov, start, passenger, chunk):
    rows, n = cov.shape
    paired = packet.shape[1] == rows
    row = lax.broadcasted_iota(jnp.int32, (SPARE, TILE if paired else n), 0)
    if not paired:
        packet[:rows, :] = cov[...]
        packet[rows:, :] = jnp.where(row == 0, passenger[...], 0.0).astype(BF16)
        return
    size = packet.shape[0] - SPARE
    other = n - rows - start
    r, c = iotas(TILE)
    for k in range(0, size, TILE):
        i = chunk * size + k
        for j in range(0, rows, TILE):
            mine = cov[i : i + TILE, pl.ds(pl.multiple_of(start + j, TILE), TILE)]
            cross = cov[i : i + TILE, pl.ds(pl.multiple_of(other + j, TILE), TILE)]
            if j > i:
                tile = mine
            elif j < i:
                tile = cross
            else:
                tile = jnp.where(c >= r, mine.astype(F32), cross.astype(F32)).astype(BF16)
                spare = jnp.where(row == 0, tile_diag(cross), 0.0)
                if passenger is not None:
                    for k_row in range(n // rows):
                        at = k_row * rows + i
                        spare = jnp.where(row == k_row + 1, passenger[:, at : at + TILE], spare)
                packet[size:, i : i + TILE] = spare.astype(BF16)
            packet[k : k + TILE, j : j + TILE] = tile


def unpack(full, diag, rider, packets, start, chunk):
    n = full.shape[0]
    if len(packets) == 1:
        (packet,) = packets
        rows = packet.shape[1] - SPARE
        for k in range(packet.shape[0]):
            full[k * rows : (k + 1) * rows, :] = packet[k, :rows, :]
        for i in range(0, n, TILE):
            diag[:, i : i + TILE] = tile_diag(full[i : i + TILE, i : i + TILE])
        rider[...] = packet[0, rows:, :].astype(F32)[0:1]
        return
    size = packets[0].shape[0] - SPARE
    rows = packets[0].shape[1]
    base = (start, n - rows - start)
    r, c = iotas(TILE)

    def put(at_row, i, at_col, j, tile):
        full[
            pl.ds(pl.multiple_of(at_row + i, TILE), TILE),
            pl.ds(pl.multiple_of(at_col + j, TILE), TILE),
        ] = tile

    for k in range(0, size, TILE):
        i = chunk * size + k
        spare = packets[0][size:, i : i + TILE].astype(F32)
        for k_row in range(n // rows):
            at = k_row * rows + i
            rider[:, at : at + TILE] = spare[k_row + 1 : k_row + 2]
        for mine, yours in ((0, 1), (1, 0)):
            for j in range(0, rows, TILE):
                tile = packets[mine][k : k + TILE, j : j + TILE]
                flip = tile.T
                if j > i:
                    put(base[mine], i, base[mine], j, tile)
                    put(base[mine], j, base[mine], i, flip)
                elif j < i:
                    put(base[mine], i, base[yours], j, tile)
                    put(base[yours], j, base[mine], i, flip)
                else:
                    tile = tile.astype(F32)
                    flip = flip.astype(F32)
                    theirs = packets[yours][k : k + TILE, i : i + TILE].T.astype(F32)
                    own = jnp.where(c >= r, tile, flip)
                    put(base[mine], i, base[mine], i, own.astype(BF16))
                    cross = jnp.where(c < r, tile, jnp.where(c > r, theirs, spare[0:1]))
                    put(base[mine], i, base[yours], i, cross.astype(BF16))
                    diag[:, pl.ds(pl.multiple_of(base[mine] + i, TILE), TILE)] = tile_diag(own)


def product_rows(cov, gram, coupling, right, start, chunk, chunks, sign):
    size = cov.shape[0] // chunks
    at = chunk * size
    here = pl.ds(pl.multiple_of(start + at, size), size)
    term = mm_t(coupling[:, here], right[...])
    cov[at : at + size, :] = (gram[at : at + size, :] + sign * term).astype(BF16)


def fold_kernel(ids, factor, lower, own, lower_a, lower_b, square, cross, sems):
    rows = factor.shape[0]
    half = rows // 2
    quarter = rows // 4
    start = pl.multiple_of(ids[0], rows)
    moves = [
        (lower.at[:half], lower_a),
        (factor, own),
        (factor.at[half:, pl.ds(start, rows)], square.at[:half]),
        (factor.at[:quarter, pl.ds(start, half)], square.at[half:, :half]),
        (factor.at[quarter:half, pl.ds(start, half)], square.at[half:, half:]),
        (factor.at[:, :rows], cross),
        (lower.at[half:], lower_b),
    ]
    copies = [pltpu.make_async_copy(s, t, sems.at[i]) for i, (s, t) in enumerate(moves)]
    for copy in copies:
        copy.start()
    for copy in copies:
        copy.wait()


def unfold(target, squares, crosses, start, sems):
    rows = squares[0].shape[0] * 4 // 3
    half = rows // 2
    quarter = rows // 4
    n = target.shape[0]
    moves = []
    for square, at in zip(squares, (start, n - rows - start)):
        moves += [
            (square.at[:half], target.at[pl.ds(at + half, half), pl.ds(at, rows)]),
            (square.at[half:, :half], target.at[pl.ds(at, quarter), pl.ds(at, half)]),
            (
                square.at[half:, half:],
                target.at[pl.ds(at + quarter, quarter), pl.ds(at, half)],
            ),
        ]
        zeros = jnp.zeros((half, half), BF16)
        target[pl.ds(at, half), pl.ds(pl.multiple_of(at + half, half), half)] = zeros
    target[:rows, rows:] = jnp.zeros((rows, n - rows), BF16)
    copies = [pltpu.make_async_copy(s, t, sems.at[i]) for i, (s, t) in enumerate(moves)]
    for copy in copies:
        copy.start()
    low = target.at[rows:, :rows]

    @pl.when(start == 0)
    def _():
        pltpu.make_async_copy(crosses[1], low, sems.at[len(moves)]).start()

    @pl.when(start != 0)
    def _():
        pltpu.make_async_copy(crosses[0], low, sems.at[len(moves)]).start()

    return copies + [pltpu.make_async_copy(crosses[0], low, sems.at[len(moves)])]


def place(target, pieces, start):
    n = target.shape[0]
    if len(pieces) == 1:
        target[...] = pieces[0][...]
        return
    rows = pieces[0].shape[0]
    for piece, at in zip(pieces, (start, n - rows - start)):
        target[pl.ds(pl.multiple_of(at, rows), rows), :] = piece[...]


def gram_kernel(pieces, ids, *refs):
    pieces, (factor, gram) = refs[:pieces], refs[pieces:]
    rows, n = gram.shape
    half = n // 2
    start = pl.multiple_of(ids[0], rows)
    own = pl.ds(start, rows)
    place(factor, pieces, start)
    gram[:, :half] = mm_t(factor[:, own], factor[:, :half])
    gram[:, half:] = mm_t(factor[half:, own], factor[half:, half:])


def first_kernel(pieces, chunks, ids, *refs):
    lowers = refs[:pieces]
    factor, gram, coupling, packet, cov = refs[pieces:]
    rows, n = cov.shape
    start = pl.multiple_of(ids[0], rows)
    size = rows // 2
    if pieces == 1:
        placed = [(lowers[0], 0)]
    else:
        first, second, other = lowers
        placed = [
            (first, start),
            (second, pl.multiple_of(start + size, size)),
            (other, pl.multiple_of(n - rows - start, rows)),
        ]
    couple(coupling, placed, factor)

    @pl.when(ids[1] == TB - 1)
    def _():
        product_rows(cov, gram, coupling, coupling, start, 0, chunks, 1)
        pack(packet, cov, start, None if chunks > 1 else jnp.zeros((1, n), F32), 0)


def rest_kernel(block, sign, ids, gram, coupling, *refs):
    packet, cov = refs[len(refs) - 2 :]
    right, passenger = (coupling, None) if len(refs) == 3 else refs[:2]
    start = pl.multiple_of(ids[0], cov.shape[0])

    @pl.when(ids[1] == block)
    def _():
        product_rows(cov, gram, coupling, right, start, 1, 2, sign)
        pack(packet, cov, start, passenger, 1)


def open_kernel(lowest, highest, ids, mine, yours, full, diag, rider):
    @pl.when(jnp.logical_and(ids[1] >= lowest, ids[1] <= highest))
    def _():
        unpack(full, diag, rider, (mine, yours), ids[0], 0)


def second_kernel(pieces, chunks, ids, *refs):
    packets = refs[:pieces]
    coupling, gram = refs[pieces : pieces + 2]
    packet, off, cov, full, diag, rider = refs[len(refs) - 6 :]
    rows = cov.shape[0]
    start = pl.multiple_of(ids[0], rows)

    @pl.when(ids[1] == TB - 2)
    def _():
        unpack(full, diag, rider, packets, start, chunks - 1)
        off[...] = (-mm(full[...], coupling[...])).astype(BF16)
        product_rows(cov, gram, coupling, off, start, 0, chunks, -1)
        pack(packet, cov, start, diag, 0)


def heard_kernel(parts, ids, *refs):
    parts, rest = refs[:parts], refs[parts:]
    (factor, coupling, cov_3, off_2, cov_2, heard, gram_1, diag_0, coupling_1, coupling_0,
     off_out, cov_out, off, sems, out_sems) = rest
    rows, _ = cov_3.shape
    start = pl.multiple_of(ids[0], rows)
    block = ids[1]

    @pl.when(block == TB - 1)
    def _():
        off[...] = -coupling[pl.ds(start, rows), :]
        write_out((off, cov_3), (off_out, cov_out), out_sems)

    @pl.when(block == TB - 2)
    def _():
        write_out((off_2.at[pl.ds(start, rows)], cov_2), (off_out, cov_out), out_sems)

    def finish(factor_1, factor_0, known):
        known[...] = coupling[...]
        gram_1[...] = mm_t(factor_1[...], factor_1[...])
        diag_0[...] = jnp.sum(jnp.square(factor_0[...].astype(F32)), axis=0, keepdims=True)

    @pl.when(block < 2)
    def _():
        if len(parts) > 1:
            for copy in unfold(heard, parts[:2], parts[2:], start, sems):
                copy.wait()
        else:
            heard[...] = parts[0][...]

        @pl.when(block == 0)
        def _():
            finish(heard, factor, coupling_0)

        @pl.when(block == 1)
        def _():
            finish(factor, heard, coupling_1)


def ready_kernel(pieces, first, ids, *refs):
    lowers, heard = refs[:pieces], refs[pieces]
    coupling_1, coupling_0 = refs[len(refs) - 2 :]
    n = heard.shape[0]
    size = lowers[0].shape[0]
    placed = [(lowers[0], 0)]
    if pieces > 1:
        bases = (ids[0], n - 2 * size - ids[0])
        placed = [(p, pl.multiple_of(b + first, size)) for p, b in zip(lowers, bases)]

    @pl.when(ids[1] == 0)
    def _():
        couple(coupling_1, placed, heard)

    @pl.when(ids[1] == 1)
    def _():
        couple(coupling_0, placed, heard)


def merge_kernel(ids, at_0, at_1, out, sem):
    block = ids[1]

    @pl.when(block == 0)
    def _():
        copy = pltpu.make_async_copy(at_0, out, sem.at[0])
        copy.start()
        copy.wait()

    @pl.when(block == 1)
    def _():
        copy = pltpu.make_async_copy(at_1, out, sem.at[0])
        copy.start()
        copy.wait()


def third_kernel(pieces, chunks, ids, *refs):
    packets = refs[:pieces]
    coupling_1, gram_1, coupling_0, diag_0 = refs[pieces : pieces + 4]
    off_0, off_1, cov_1, variances, full, diag, rider = refs[len(refs) - 7 :]
    n = full.shape[0]

    @pl.when(ids[1] < 2)
    def _():
        unpack(full, diag, rider, packets, ids[0], chunks - 1)
        var_2 = diag[...]
        var_3 = rider[...]
        off_1[...] = (-mm(full[...], coupling_1[...])).astype(BF16)
        cov_1[...] = (gram_1[...] - mm_t(coupling_1[...], off_1[...])).astype(BF16)
        off_0[...] = (-mm(cov_1[...], coupling_0[...])).astype(BF16)
        for i in range(0, n, TILE):
            diag[:, i : i + TILE] = tile_diag(cov_1[i : i + TILE, i : i + TILE])
        product = coupling_0[...].astype(F32) * off_0[...].astype(F32)
        var_0 = diag_0[...] - jnp.sum(product, axis=0, keepdims=True)
        row = lax.broadcasted_iota(jnp.int32, variances.shape, 0)
        merged = jnp.where(row == 0, var_0, jnp.where(row == 1, diag[...], 0.0))
        merged = jnp.where(row == 2, var_2, jnp.where(row == 3, var_3, merged))
        variances[...] = merged.astype(BF16)


def last_kernel(ids, coupling_0, gram, off_0, off_1, cov_1, _, __, off_out, cov_out, cov, sems):
    rows = cov.shape[0]
    start = pl.multiple_of(ids[0], rows)
    block = ids[1]
    own = pl.ds(start, rows)

    @pl.when(block == 1)
    def _():
        one = pltpu.make_async_copy(off_1.at[own], off_out, sems.at[0])
        two = pltpu.make_async_copy(cov_1.at[own], cov_out, sems.at[1])
        one.start()
        two.start()
        one.wait()
        two.wait()

    @pl.when(block == 0)
    def _():
        one = pltpu.make_async_copy(off_0.at[own], off_out, sems.at[0])
        one.start()
        copies = [one]
        parts = 2 if rows % (2 * TILE) == 0 else 1
        for k in range(parts):
            product_rows(cov, gram, coupling_0, off_0, start, k, parts, -1)
            here = pl.ds(k * rows // parts, rows // parts)
            copies.append(
                pltpu.make_async_copy(cov.at[here], cov_out.at[here], sems.at[k + 1])
            )
            copies[-1].start()
        for copy in copies:
            copy.wait()


def deliver_kernel(ids, owner, mine, heard, out):
    block = ids[1]
    dev = ids[2]
    values = jnp.where(block < 2, mine[...].astype(F32), heard[...].astype(F32))
    lines = [jnp.zeros((1, out.shape[1]), F32) for _ in range(SLOTS)]
    for t in range(TB):
        rank = jnp.int32(0)
        for before in range(t):
            rank += (owner[before] == owner[t]).astype(jnp.int32)
        for slot in range(SLOTS):
            here = jnp.logical_and(owner[t] == dev, rank == slot)
            lines[slot] += jnp.where(here, values[t : t + 1], 0.0)
    for slot in range(SLOTS):
        out[slot : slot + 1, :] = lines[slot]


def shards(linv, sub, owner):
    group = lax.axis_size("tm") // TB
    rows, n = linv.shape
    paired = group == 2
    dev = lax.axis_index("tm")
    member = dev % group

    def block_to_block(values, routes, members=range(group)):
        pairs = [(s * group + i, t * group + i) for s, t in routes for i in members]
        return lax.ppermute(values, "tm", pairs)

    def peer(piece, step=1):
        return lax.ppermute(piece, "tm", [(i, i ^ step) for i in range(TB * group)])

    def pieces_of(piece):
        if paired:
            return [piece, peer(piece)]
        step = 1
        while step < group:
            other = peer(piece, step)
            upper = (member // step) % 2 == 1
            piece = jnp.concatenate(
                [jnp.where(upper, other, piece), jnp.where(upper, piece, other)], 0
            )
            step *= 2
        return [piece]

    def packets_of(packet):
        return pieces_of(packet) if paired else pieces_of(packet[None])

    def after(values, *others):
        return lax.optimization_barrier((values, *others))[0]

    def call(kernel, out, inputs, spaces, scratch, aliases=None):
        shapes = tuple(
            pltpu.HBM(o[1], o[2]) if o[0] is HBM else pltpu.VMEM(o[1], o[2]) for o in out
        )
        placed = [
            x if space is SMEM else pltpu.with_memory_space_constraint(x, space.memory_space)
            for x, space in zip(inputs, spaces, strict=True)
        ]
        return pl.pallas_call(
            located(kernel, rows, group),
            out_shape=shapes,
            in_specs=list(spaces),
            out_specs=tuple(o[0] for o in out),
            scratch_shapes=scratch,
            input_output_aliases=aliases or {},
            compiler_params=PARAMS,
        )(*placed)

    def sems(*shape):
        return pltpu.SemaphoreType.DMA(shape)

    pieces = 2 if paired else 1
    chunks = 2 if paired else 1
    size = rows // chunks
    packet_shape = (size + SPARE, rows if paired else n)
    whole = (VMEM, (n, n), BF16)
    part = (VMEM, (rows, n), BF16)
    line = (VMEM, (1, n), F32)
    packed = (VMEM, packet_shape, BF16)
    out_rows = (HBM, (rows, n), BF16)

    def swapped(piece, *others):
        return pieces_of(after(piece, *others) if others else piece)

    swap = [(1, 0), (0, 1)]
    if paired:
        other_factor, other_lower = peer(linv), peer(sub)
        half_rows = (VMEM, (size, n), BF16)
        own, lower_a, lower_b, square, cross = call(
            fold_kernel,
            [part, half_rows, half_rows,
             (VMEM, (rows * 3 // 4, rows), BF16), (VMEM, (rows, rows), BF16)],
            [linv, sub],
            [HBM, HBM],
            [sems(7)],
        )
        factors = [own, other_factor]
        lowers = [lower_a, lower_b, other_lower]
        raw_lower = [block_to_block(lower_a, swap), block_to_block(lower_b, swap)]
        raw_factor = [
            block_to_block(square, swap), block_to_block(cross, swap, range(1, 2))
        ]
    else:
        factors = pieces_of(linv)
        lowers = pieces_of(sub)
        raw_lower = [block_to_block(sub, swap)]
        raw_factor = [block_to_block(linv, swap)]

    factor, gram = call(
        functools.partial(gram_kernel, pieces),
        [whole, (VMEM, (rows, n), F32)],
        [*factors],
        [VMEM] * pieces,
        [],
    )
    coupling, packet_a, cov_3 = call(
        functools.partial(first_kernel, len(lowers), chunks),
        [whole, packed, part],
        [*lowers, factor, gram],
        [VMEM] * (len(lowers) + 2),
        [],
    )
    packets_2 = [block_to_block(packet_a, [(3, 2)])]
    if chunks > 1:
        packet_b, cov_3 = call(
            functools.partial(rest_kernel, TB - 1, 1),
            [packed, part],
            [gram, coupling, cov_3],
            [VMEM] * 3,
            [],
            {2: 1},
        )
        packets_2.append(block_to_block(packet_b, [(3, 2)]))

    opened = []
    if chunks > 1:
        opened = call(
            functools.partial(open_kernel, 2, 2),
            [whole, line, line],
            [*packets_of(packets_2[0])],
            [VMEM, VMEM],
            [],
        )
    packet_a, off_2, cov_2, _, diag_2, _ = call(
        functools.partial(second_kernel, pieces, chunks),
        [packed, whole, part, whole, line, line],
        [*packets_of(packets_2[-1]), coupling, gram, *opened],
        [VMEM] * (pieces + 2 + len(opened)),
        [],
        {pieces + 2 + i: 3 + i for i in range(len(opened))},
    )
    packet = packet_a
    packets_0 = [block_to_block(packet_a, [(2, 0)])]
    packets_1 = [block_to_block(packet_a, [(2, 1)])]
    if chunks > 1:
        packet, cov_2 = call(
            functools.partial(rest_kernel, TB - 2, -1),
            [packed, part],
            [gram, coupling, off_2, diag_2, cov_2],
            [VMEM] * 5,
            [],
            {4: 1},
        )
        packets_0.append(block_to_block(packet, [(2, 0)]))
        packets_1.append(block_to_block(packet, [(2, 1)]))

    parts = [x for piece in raw_factor for x in swapped(piece, packet)]
    heard_factor, gram_1, diag_0, coupling_1, coupling_0, off_rows, cov_rows = call(
        functools.partial(heard_kernel, len(parts)),
        [whole, (VMEM, (n, n), F32), line, whole, whole, out_rows, out_rows],
        [*parts, factor, coupling, cov_3, off_2, cov_2],
        [VMEM] * (len(parts) + 5),
        [pltpu.VMEM((rows, n), BF16), sems(8), sems(2)],
    )
    for k, piece in enumerate(raw_lower):
        coupling_1, coupling_0 = call(
            functools.partial(ready_kernel, pieces, k * size),
            [whole, whole],
            [*swapped(piece, packet), heard_factor,
             coupling_1, coupling_0],
            [VMEM] * (pieces + 3),
            [],
            {pieces + 1: 0, pieces + 2: 1},
        )

    carried = [
        call(merge_kernel, [packed], [at_0, at_1], [VMEM, VMEM], [sems(1)])[0]
        for at_0, at_1 in zip(packets_0, packets_1)
    ]
    opened = []
    if chunks > 1:
        opened = call(
            functools.partial(open_kernel, 0, 1),
            [whole, line, line],
            [*packets_of(carried[0])],
            [VMEM, VMEM],
            [],
        )
    off_0, off_1, cov_1, variances, *_ = call(
        functools.partial(third_kernel, pieces, chunks),
        [whole, whole, whole, (VMEM, (SPARE, n), BF16), whole, line, line],
        [*packets_of(carried[-1]), coupling_1, gram_1, coupling_0, diag_0,
         *opened],
        [VMEM] * (pieces + 4 + len(opened)),
        [],
        {pieces + 4 + i: 4 + i for i in range(len(opened))},
    )
    heard = block_to_block(variances, [(0, 2), (1, 3)])

    off_rows, cov_rows = call(
        last_kernel,
        [out_rows, out_rows],
        [coupling_0, gram, off_0, off_1, cov_1, off_rows, cov_rows],
        [VMEM] * 5 + [HBM, HBM],
        [pltpu.VMEM((rows, n), BF16), sems(3)],
        {5: 0, 6: 1},
    )
    (owned_var,) = call(
        deliver_kernel,
        [(VMEM, (SLOTS, n), F32)],
        [owner, variances, heard],
        [SMEM, VMEM, VMEM],
        [],
    )
    return (cov_rows, off_rows, owned_var)


def solution(mesh):
    return jax.shard_map(
        shards,
        mesh=mesh,
        in_specs=(P(("cfg", "tm"), None), P(("cfg", "tm"), None), P("cfg")),
        out_specs=(P(("cfg", "tm"), None), P(("cfg", "tm"), None), P(("cfg", "tm"), None)),
        check_vma=False,
    )
```

```python
import functools

import jax
import jax.numpy as jnp
from jax import lax
from jax.experimental import pallas as pl
from jax.experimental.pallas import tpu as pltpu
from jax.sharding import PartitionSpec as P


TB = 4
SLOTS = 2
SPARE = 16
TILE = 128

CONTRACT_FIRST = (((0,), (0,)), ((), ()))
BF16 = jnp.bfloat16
F32 = jnp.float32

HBM = pl.BlockSpec(memory_space=pltpu.HBM)
VMEM = pl.BlockSpec(memory_space=pltpu.VMEM)
SMEM = pl.BlockSpec(memory_space=pltpu.SMEM)
PARAMS = pltpu.CompilerParams(vmem_limit_bytes=18 << 20)


def located(kernel, rows, group):
    def body(*refs):
        dev = lax.axis_index("tm")
        member = lax.rem(dev, jnp.int32(group))
        kernel((member * rows, lax.div(dev, jnp.int32(group)), dev), *refs)

    return body


def mm(a, b):
    return jnp.dot(a, b, preferred_element_type=F32)


def mm_t(a, b):
    return lax.dot_general(a, b, CONTRACT_FIRST, preferred_element_type=F32)


def iotas(size):
    r = lax.broadcasted_iota(jnp.int32, (size, size), 0)
    c = lax.broadcasted_iota(jnp.int32, (size, size), 1)
    return r, c


def couple(target, lowers, factor):
    half = factor.shape[0] // 2
    for lower, at in lowers:
        here = pl.ds(at, lower.shape[0])
        target[here, :half] = mm(lower[...], factor[:, :half]).astype(BF16)
        target[here, half:] = mm(lower[:, half:], factor[half:, half:]).astype(BF16)


def write_out(values, outs, sems):
    copies = [
        pltpu.make_async_copy(v, o, sems.at[i]) for i, (v, o) in enumerate(zip(values, outs))
    ]
    for copy in copies:
        copy.start()
    for copy in copies:
        copy.wait()


def tile_diag(tile):
    r, c = iotas(TILE)
    return jnp.sum(jnp.where(r == c, tile.astype(F32), 0.0), axis=0, keepdims=True)


def pack(packet, cov, start, passenger, chunk):
    rows, n = cov.shape
    paired = packet.shape[1] == rows
    row = lax.broadcasted_iota(jnp.int32, (SPARE, TILE if paired else n), 0)
    if not paired:
        packet[:rows, :] = cov[...]
        packet[rows:, :] = jnp.where(row == 0, passenger[...], 0.0).astype(BF16)
        return
    size = packet.shape[0] - SPARE
    other = n - rows - start
    r, c = iotas(TILE)
    for k in range(0, size, TILE):
        i = chunk * size + k
        for j in range(0, rows, TILE):
            mine = cov[i : i + TILE, pl.ds(pl.multiple_of(start + j, TILE), TILE)]
            cross = cov[i : i + TILE, pl.ds(pl.multiple_of(other + j, TILE), TILE)]
            if j > i:
                tile = mine
            elif j < i:
                tile = cross
            else:
                tile = jnp.where(c >= r, mine.astype(F32), cross.astype(F32)).astype(BF16)
                spare = jnp.where(row == 0, tile_diag(cross), 0.0)
                if passenger is not None:
                    for k_row in range(n // rows):
                        at = k_row * rows + i
                        spare = jnp.where(row == k_row + 1, passenger[:, at : at + TILE], spare)
                packet[size:, i : i + TILE] = spare.astype(BF16)
            packet[k : k + TILE, j : j + TILE] = tile


def unpack(full, diag, rider, packets, start, chunk):
    n = full.shape[0]
    if len(packets) == 1:
        (packet,) = packets
        rows = packet.shape[1] - SPARE
        for k in range(packet.shape[0]):
            full[k * rows : (k + 1) * rows, :] = packet[k, :rows, :]
        for i in range(0, n, TILE):
            diag[:, i : i + TILE] = tile_diag(full[i : i + TILE, i : i + TILE])
        rider[...] = packet[0, rows:, :].astype(F32)[0:1]
        return
    size = packets[0].shape[0] - SPARE
    rows = packets[0].shape[1]
    base = (start, n - rows - start)
    r, c = iotas(TILE)

    def put(at_row, i, at_col, j, tile):
        full[
            pl.ds(pl.multiple_of(at_row + i, TILE), TILE),
            pl.ds(pl.multiple_of(at_col + j, TILE), TILE),
        ] = tile

    for k in range(0, size, TILE):
        i = chunk * size + k
        spare = packets[0][size:, i : i + TILE].astype(F32)
        for k_row in range(n // rows):
            at = k_row * rows + i
            rider[:, at : at + TILE] = spare[k_row + 1 : k_row + 2]
        for mine, yours in ((0, 1), (1, 0)):
            for j in range(0, rows, TILE):
                tile = packets[mine][k : k + TILE, j : j + TILE]
                flip = tile.T
                if j > i:
                    put(base[mine], i, base[mine], j, tile)
                    put(base[mine], j, base[mine], i, flip)
                elif j < i:
                    put(base[mine], i, base[yours], j, tile)
                    put(base[yours], j, base[mine], i, flip)
                else:
                    tile = tile.astype(F32)
                    flip = flip.astype(F32)
                    theirs = packets[yours][k : k + TILE, i : i + TILE].T.astype(F32)
                    own = jnp.where(c >= r, tile, flip)
                    put(base[mine], i, base[mine], i, own.astype(BF16))
                    cross = jnp.where(c < r, tile, jnp.where(c > r, theirs, spare[0:1]))
                    put(base[mine], i, base[yours], i, cross.astype(BF16))
                    diag[:, pl.ds(pl.multiple_of(base[mine] + i, TILE), TILE)] = tile_diag(own)


def product_rows(cov, gram, coupling, right, start, chunk, chunks, sign):
    size = cov.shape[0] // chunks
    at = chunk * size
    here = pl.ds(pl.multiple_of(start + at, size), size)
    term = mm_t(coupling[:, here], right[...])
    cov[at : at + size, :] = (gram[at : at + size, :] + sign * term).astype(BF16)


def strips(rows):
    return [(k * TILE, (k + 1) * TILE, k * (k + 1) // 2 * TILE) for k in range(rows // TILE)]


def fold_kernel(ids, factor, lower, own, lower_a, lower_b, square, cross, sems):
    rows = factor.shape[0]
    cut = lower_a.shape[0]
    start = pl.multiple_of(ids[0], rows)
    moves = [(factor, own)]
    for row, width, at in strips(rows):
        moves.append(
            (factor.at[row : row + TILE, pl.ds(start, width)], square.at[:, at : at + width])
        )
    moves += [
        (lower.at[:cut], lower_a),
        (lower.at[cut:], lower_b),
        (factor.at[:, :rows], cross),
    ]
    copies = [pltpu.make_async_copy(s, t, sems.at[i]) for i, (s, t) in enumerate(moves)]
    for copy in copies:
        copy.start()
    for copy in copies:
        copy.wait()


def unfold(target, squares, crosses, start, sems):
    n = target.shape[0]
    rows = n // 2
    moves = []
    for square, base in zip(squares, (start, n - rows - start)):
        for row, width, at in strips(rows):
            here = pl.ds(pl.multiple_of(base + row, TILE), TILE)
            cols = pl.ds(pl.multiple_of(base, rows), width)
            moves.append((square.at[:, at : at + width], target.at[here, cols]))
            if width < rows:
                rest = pl.ds(pl.multiple_of(base + width, TILE), rows - width)
                target[here, rest] = jnp.zeros((TILE, rows - width), BF16)
    target[:rows, rows:] = jnp.zeros((rows, n - rows), BF16)
    copies = [pltpu.make_async_copy(s, t, sems.at[i]) for i, (s, t) in enumerate(moves)]
    for copy in copies:
        copy.start()
    low = target.at[rows:, :rows]

    @pl.when(start == 0)
    def _():
        pltpu.make_async_copy(crosses[1], low, sems.at[len(moves)]).start()

    @pl.when(start != 0)
    def _():
        pltpu.make_async_copy(crosses[0], low, sems.at[len(moves)]).start()

    return copies + [pltpu.make_async_copy(crosses[0], low, sems.at[len(moves)])]


def place(target, pieces, start):
    n = target.shape[0]
    if len(pieces) == 1:
        target[...] = pieces[0][...]
        return
    rows = pieces[0].shape[0]
    for piece, at in zip(pieces, (start, n - rows - start)):
        target[pl.ds(pl.multiple_of(at, rows), rows), :] = piece[...]


def gram_kernel(pieces, ids, *refs):
    pieces, (factor, gram) = refs[:pieces], refs[pieces:]
    rows, n = gram.shape
    half = n // 2
    start = pl.multiple_of(ids[0], rows)
    own = pl.ds(start, rows)
    place(factor, pieces, start)
    gram[:, :half] = mm_t(factor[:, own], factor[:, :half])
    gram[:, half:] = mm_t(factor[half:, own], factor[half:, half:])


def first_kernel(pieces, chunks, ids, *refs):
    lowers = refs[:pieces]
    factor, gram, coupling, packet, cov = refs[pieces:]
    rows, n = cov.shape
    start = pl.multiple_of(ids[0], rows)
    if pieces == 1:
        placed = [(lowers[0], 0)]
    else:
        first, second, other = lowers
        placed = [
            (first, start),
            (second, pl.multiple_of(start + first.shape[0], TILE)),
            (other, pl.multiple_of(n - rows - start, rows)),
        ]
    couple(coupling, placed, factor)

    @pl.when(ids[1] == TB - 1)
    def _():
        product_rows(cov, gram, coupling, coupling, start, 0, chunks, 1)
        pack(packet, cov, start, None if chunks > 1 else jnp.zeros((1, n), F32), 0)


def rest_kernel(block, sign, ids, gram, coupling, *refs):
    packet, cov = refs[len(refs) - 2 :]
    right, passenger = (coupling, None) if len(refs) == 3 else refs[:2]
    start = pl.multiple_of(ids[0], cov.shape[0])

    @pl.when(ids[1] == block)
    def _():
        product_rows(cov, gram, coupling, right, start, 1, 2, sign)
        pack(packet, cov, start, passenger, 1)


def open_kernel(lowest, highest, ids, mine, yours, full, diag, rider):
    @pl.when(jnp.logical_and(ids[1] >= lowest, ids[1] <= highest))
    def _():
        unpack(full, diag, rider, (mine, yours), ids[0], 0)


def second_kernel(pieces, chunks, ids, *refs):
    packets = refs[:pieces]
    coupling, gram = refs[pieces : pieces + 2]
    packet, off, cov, full, diag, rider = refs[len(refs) - 6 :]
    rows = cov.shape[0]
    start = pl.multiple_of(ids[0], rows)

    @pl.when(ids[1] == TB - 2)
    def _():
        unpack(full, diag, rider, packets, start, chunks - 1)
        off[...] = (-mm(full[...], coupling[...])).astype(BF16)
        product_rows(cov, gram, coupling, off, start, 0, chunks, -1)
        pack(packet, cov, start, diag, 0)


def heard_kernel(parts, ids, *refs):
    parts, rest = refs[:parts], refs[parts:]
    (factor, coupling, cov_3, off_2, cov_2, heard, gram_1, diag_0, coupling_1, coupling_0,
     off_out, cov_out, off, sems, out_sems) = rest
    rows, _ = cov_3.shape
    start = pl.multiple_of(ids[0], rows)
    block = ids[1]

    @pl.when(block == TB - 1)
    def _():
        off[...] = -coupling[pl.ds(start, rows), :]
        write_out((off, cov_3), (off_out, cov_out), out_sems)

    @pl.when(block == TB - 2)
    def _():
        write_out((off_2.at[pl.ds(start, rows)], cov_2), (off_out, cov_out), out_sems)

    def finish(factor_1, factor_0, known):
        known[...] = coupling[...]
        gram_1[...] = mm_t(factor_1[...], factor_1[...])
        diag_0[...] = jnp.sum(jnp.square(factor_0[...].astype(F32)), axis=0, keepdims=True)

    @pl.when(block < 2)
    def _():
        if len(parts) > 1:
            for copy in unfold(heard, parts[:2], parts[2:], start, sems):
                copy.wait()
        else:
            heard[...] = parts[0][...]

        @pl.when(block == 0)
        def _():
            finish(heard, factor, coupling_0)

        @pl.when(block == 1)
        def _():
            finish(factor, heard, coupling_1)


def ready_kernel(pieces, rows, first, ids, *refs):
    lowers, heard = refs[:pieces], refs[pieces]
    coupling_1, coupling_0 = refs[len(refs) - 2 :]
    n = heard.shape[0]
    placed = [(lowers[0], 0)]
    if pieces > 1:
        bases = (ids[0], n - rows - ids[0])
        placed = [(p, pl.multiple_of(b + first, TILE)) for p, b in zip(lowers, bases)]

    @pl.when(ids[1] == 0)
    def _():
        couple(coupling_1, placed, heard)

    @pl.when(ids[1] == 1)
    def _():
        couple(coupling_0, placed, heard)


def merge_kernel(ids, at_0, at_1, out, sem):
    block = ids[1]

    @pl.when(block == 0)
    def _():
        copy = pltpu.make_async_copy(at_0, out, sem.at[0])
        copy.start()
        copy.wait()

    @pl.when(block == 1)
    def _():
        copy = pltpu.make_async_copy(at_1, out, sem.at[0])
        copy.start()
        copy.wait()


def third_kernel(pieces, chunks, ids, *refs):
    packets = refs[:pieces]
    coupling_1, gram_1, coupling_0, diag_0 = refs[pieces : pieces + 4]
    off_0, off_1, cov_1, variances, full, diag, rider = refs[len(refs) - 7 :]
    n = full.shape[0]

    @pl.when(ids[1] < 2)
    def _():
        unpack(full, diag, rider, packets, ids[0], chunks - 1)
        var_2 = diag[...]
        var_3 = rider[...]
        off_1[...] = (-mm(full[...], coupling_1[...])).astype(BF16)
        cov_1[...] = (gram_1[...] - mm_t(coupling_1[...], off_1[...])).astype(BF16)
        for i in range(0, n, TILE):
            diag[:, i : i + TILE] = tile_diag(cov_1[i : i + TILE, i : i + TILE])
        off_0[...] = (-mm(cov_1[...], coupling_0[...])).astype(BF16)
        product = coupling_0[...].astype(F32) * off_0[...].astype(F32)
        var_0 = diag_0[...] - jnp.sum(product, axis=0, keepdims=True)
        row = lax.broadcasted_iota(jnp.int32, variances.shape, 0)
        merged = jnp.where(row == 0, var_0, jnp.where(row == 1, diag[...], 0.0))
        merged = jnp.where(row == 2, var_2, jnp.where(row == 3, var_3, merged))
        variances[...] = merged.astype(BF16)


def owned_lines(mask, variances):
    values = variances[...].astype(F32)
    lines = []
    for slot in range(SLOTS):
        line = jnp.zeros((1, values.shape[1]), F32)
        for t in range(TB):
            at = slot * TB + t
            line += jnp.where(mask[at : at + 1, :] > 0, values[t : t + 1], 0.0)
        lines.append(line)
    return lines


def choose_kernel(ids, owner, mask):
    for t in range(TB):
        rank = jnp.int32(0)
        for before in range(t):
            rank += (owner[before] == owner[t]).astype(jnp.int32)
        for slot in range(SLOTS):
            here = jnp.logical_and(owner[t] == ids[2], rank == slot)
            at = slot * TB + t
            mask[at : at + 1, :] = jnp.full((1, mask.shape[1]), jnp.where(here, 1.0, 0.0), F32)


def last_kernel(ids, coupling_0, gram, off_0, off_1, cov_1, variances, mask, _, __,
                off_out, cov_out, own_out, cov, lines, sems):
    rows = cov.shape[0]
    start = pl.multiple_of(ids[0], rows)
    block = ids[1]
    own = pl.ds(start, rows)

    def begin(source, target, sem):
        copy = pltpu.make_async_copy(source, target, sems.at[sem])
        copy.start()
        return copy

    def owned():
        for slot, line in enumerate(owned_lines(mask, variances)):
            lines[slot : slot + 1, :] = line
        return begin(lines, own_out, 0)

    @pl.when(block == 1)
    def _():
        copies = [begin(off_1.at[own], off_out, 1), begin(cov_1.at[own], cov_out, 2), owned()]
        for copy in copies:
            copy.wait()

    @pl.when(block == 0)
    def _():
        copies = [begin(off_0.at[own], off_out, 1), owned()]
        parts = 2 if rows % (2 * TILE) == 0 else 1
        for k in range(parts):
            product_rows(cov, gram, coupling_0, off_0, start, k, parts, -1)
            here = pl.ds(k * rows // parts, rows // parts)
            copies.append(begin(cov.at[here], cov_out.at[here], k + 2))
        for copy in copies:
            copy.wait()


def deliver_kernel(ids, mask, heard, _, own_out, lines, sems):
    @pl.when(ids[1] >= 2)
    def _():
        for slot, line in enumerate(owned_lines(mask, heard)):
            lines[slot : slot + 1, :] = line
        copy = pltpu.make_async_copy(lines, own_out, sems.at[0])
        copy.start()
        copy.wait()


def shards(linv, sub, owner):
    group = lax.axis_size("tm") // TB
    rows, n = linv.shape
    paired = group == 2
    dev = lax.axis_index("tm")
    member = dev % group

    def block_to_block(values, routes, members=range(group)):
        pairs = [(s * group + i, t * group + i) for s, t in routes for i in members]
        return lax.ppermute(values, "tm", pairs)

    def peer(piece, step=1):
        return lax.ppermute(piece, "tm", [(i, i ^ step) for i in range(TB * group)])

    def pieces_of(piece):
        if paired:
            return [piece, peer(piece)]
        step = 1
        while step < group:
            other = peer(piece, step)
            upper = (member // step) % 2 == 1
            piece = jnp.concatenate(
                [jnp.where(upper, other, piece), jnp.where(upper, piece, other)], 0
            )
            step *= 2
        return [piece]

    def packets_of(packet):
        return pieces_of(packet) if paired else pieces_of(packet[None])

    def after(values, *others):
        return lax.optimization_barrier((values, *others))[0]

    def call(kernel, out, inputs, spaces, scratch, aliases=None):
        shapes = tuple(
            pltpu.HBM(o[1], o[2]) if o[0] is HBM else pltpu.VMEM(o[1], o[2]) for o in out
        )
        placed = [
            x if space is SMEM else pltpu.with_memory_space_constraint(x, space.memory_space)
            for x, space in zip(inputs, spaces, strict=True)
        ]
        return pl.pallas_call(
            located(kernel, rows, group),
            out_shape=shapes,
            in_specs=list(spaces),
            out_specs=tuple(o[0] for o in out),
            scratch_shapes=scratch,
            input_output_aliases=aliases or {},
            compiler_params=PARAMS,
        )(*placed)

    def sems(*shape):
        return pltpu.SemaphoreType.DMA(shape)

    pieces = 2 if paired else 1
    chunks = 2 if paired else 1
    size = rows // chunks
    packet_shape = (size + SPARE, rows if paired else n)
    whole = (VMEM, (n, n), BF16)
    part = (VMEM, (rows, n), BF16)
    line = (VMEM, (1, n), F32)
    packed = (VMEM, packet_shape, BF16)
    out_rows = (HBM, (rows, n), BF16)

    def swapped(piece, *others):
        return pieces_of(after(piece, *others) if others else piece)

    swap = [(1, 0), (0, 1)]
    if paired:
        other_factor, other_lower = peer(linv), peer(sub)
        cut = rows // 2
        own, lower_a, lower_b, square, cross = call(
            fold_kernel,
            [part, (VMEM, (cut, n), BF16), (VMEM, (rows - cut, n), BF16),
             (VMEM, (TILE, sum(w for _, w, _ in strips(rows))), BF16),
             (VMEM, (rows, rows), BF16)],
            [linv, sub],
            [HBM, HBM],
            [sems(4 + len(strips(rows)))],
        )
        factors = [own, other_factor]
        lowers = [lower_a, lower_b, other_lower]
        raw_lower = [block_to_block(lower_a, swap), block_to_block(lower_b, swap)]
        raw_factor = [block_to_block(square, swap), block_to_block(cross, swap, range(1, 2))]
    else:
        factors = pieces_of(linv)
        lowers = pieces_of(sub)
        raw_lower = [block_to_block(sub, swap)]
        raw_factor = [block_to_block(linv, swap)]

    factor, gram = call(
        functools.partial(gram_kernel, pieces),
        [whole, (VMEM, (rows, n), F32)],
        [*factors],
        [VMEM] * pieces,
        [],
    )
    coupling, packet_a, cov_3 = call(
        functools.partial(first_kernel, len(lowers), chunks),
        [whole, packed, part],
        [*lowers, factor, gram],
        [VMEM] * (len(lowers) + 2),
        [],
    )
    packets_2 = [block_to_block(packet_a, [(3, 2)])]
    if chunks > 1:
        packet_b, cov_3 = call(
            functools.partial(rest_kernel, TB - 1, 1),
            [packed, part],
            [gram, coupling, cov_3],
            [VMEM] * 3,
            [],
            {2: 1},
        )
        packets_2.append(block_to_block(packet_b, [(3, 2)]))

    (mask,) = call(choose_kernel, [(VMEM, (SLOTS * TB, n), F32)], [owner], [SMEM], [])

    opened = []
    if chunks > 1:
        opened = call(
            functools.partial(open_kernel, 2, 2),
            [whole, line, line],
            [*packets_of(packets_2[0])],
            [VMEM, VMEM],
            [],
        )
    packet_a, off_2, cov_2, _, diag_2, _ = call(
        functools.partial(second_kernel, pieces, chunks),
        [packed, whole, part, whole, line, line],
        [*packets_of(packets_2[-1]), coupling, gram, *opened],
        [VMEM] * (pieces + 2 + len(opened)),
        [],
        {pieces + 2 + i: 3 + i for i in range(len(opened))},
    )
    packet = packet_a
    packets_0 = [block_to_block(packet_a, [(2, 0)])]
    packets_1 = [block_to_block(packet_a, [(2, 1)])]
    if chunks > 1:
        packet, cov_2 = call(
            functools.partial(rest_kernel, TB - 2, -1),
            [packed, part],
            [gram, coupling, off_2, diag_2, cov_2],
            [VMEM] * 5,
            [],
            {4: 1},
        )
        packets_0.append(block_to_block(packet, [(2, 0)]))
        packets_1.append(block_to_block(packet, [(2, 1)]))

    parts = [x for piece in raw_factor for x in swapped(piece, packet)]
    heard_factor, gram_1, diag_0, coupling_1, coupling_0, off_rows, cov_rows = call(
        functools.partial(heard_kernel, len(parts)),
        [whole, (VMEM, (n, n), F32), line, whole, whole, out_rows, out_rows],
        [*parts, factor, coupling, cov_3, off_2, cov_2],
        [VMEM] * (len(parts) + 5),
        [pltpu.VMEM((rows, n), BF16), sems(2 * (rows // TILE) + 1), sems(2)],
    )
    for k, piece in enumerate(raw_lower):
        coupling_1, coupling_0 = call(
            functools.partial(ready_kernel, pieces, rows, k * rows // 2),
            [whole, whole],
            [*swapped(piece, packet), heard_factor,
             coupling_1, coupling_0],
            [VMEM] * (pieces + 3),
            [],
            {pieces + 1: 0, pieces + 2: 1},
        )

    carried = [
        call(merge_kernel, [packed], [at_0, at_1], [VMEM, VMEM], [sems(1)])[0]
        for at_0, at_1 in zip(packets_0, packets_1)
    ]
    opened = []
    if chunks > 1:
        opened = call(
            functools.partial(open_kernel, 0, 1),
            [whole, line, line],
            [*packets_of(carried[0])],
            [VMEM, VMEM],
            [],
        )
    off_0, off_1, cov_1, variances, *_ = call(
        functools.partial(third_kernel, pieces, chunks),
        [whole, whole, whole, (VMEM, (SPARE, n), BF16), whole, line, line],
        [*packets_of(carried[-1]), coupling_1, gram_1, coupling_0, diag_0,
         *opened],
        [VMEM] * (pieces + 4 + len(opened)),
        [],
        {pieces + 4 + i: 4 + i for i in range(len(opened))},
    )
    heard = block_to_block(variances, [(0, 2), (1, 3)])

    own_rows = (HBM, (SLOTS, n), F32)
    lines = pltpu.VMEM((SLOTS, n), F32)
    off_rows, cov_rows, owned_var = call(
        last_kernel,
        [out_rows, out_rows, own_rows],
        [coupling_0, gram, off_0, off_1, cov_1, variances, mask, off_rows, cov_rows],
        [VMEM] * 7 + [HBM, HBM],
        [pltpu.VMEM((rows, n), BF16), lines, sems(4)],
        {7: 0, 8: 1},
    )
    (owned_var,) = call(
        deliver_kernel,
        [own_rows],
        [mask, heard, owned_var],
        [VMEM, VMEM, HBM],
        [lines, sems(1)],
        {2: 0},
    )
    return (cov_rows, off_rows, owned_var)


def solution(mesh):
    return jax.shard_map(
        shards,
        mesh=mesh,
        in_specs=(P(("cfg", "tm"), None), P(("cfg", "tm"), None), P("cfg")),
        out_specs=(P(("cfg", "tm"), None), P(("cfg", "tm"), None), P(("cfg", "tm"), None)),
        check_vma=False,
    )
```

```python
import functools

import jax
import jax.numpy as jnp
from jax import lax
from jax.experimental import pallas as pl
from jax.experimental.pallas import tpu as pltpu
from jax.sharding import PartitionSpec as P


TB = 4
SLOTS = 2
SPARE = 16
TILE = 128

CONTRACT_FIRST = (((0,), (0,)), ((), ()))
BF16 = jnp.bfloat16
F32 = jnp.float32

HBM = pl.BlockSpec(memory_space=pltpu.HBM)
VMEM = pl.BlockSpec(memory_space=pltpu.VMEM)
SMEM = pl.BlockSpec(memory_space=pltpu.SMEM)
PARAMS = pltpu.CompilerParams(vmem_limit_bytes=18 << 20)


def located(kernel, rows, group):
    def body(*refs):
        dev = lax.axis_index("tm")
        member = lax.rem(dev, jnp.int32(group))
        kernel((member * rows, lax.div(dev, jnp.int32(group)), dev), *refs)

    return body


def mm(a, b):
    return jnp.dot(a, b, preferred_element_type=F32)


def mm_t(a, b):
    return lax.dot_general(a, b, CONTRACT_FIRST, preferred_element_type=F32)


def iotas(size):
    r = lax.broadcasted_iota(jnp.int32, (size, size), 0)
    c = lax.broadcasted_iota(jnp.int32, (size, size), 1)
    return r, c


def couple(target, lowers, factor):
    half = factor.shape[0] // 2
    for lower, at in lowers:
        here = pl.ds(at, lower.shape[0])
        target[here, :half] = mm(lower[...], factor[:, :half]).astype(BF16)
        target[here, half:] = mm(lower[:, half:], factor[half:, half:]).astype(BF16)


def write_out(values, outs, sems):
    copies = [
        pltpu.make_async_copy(v, o, sems.at[i]) for i, (v, o) in enumerate(zip(values, outs))
    ]
    for copy in copies:
        copy.start()
    for copy in copies:
        copy.wait()


def tile_diag(tile):
    r, c = iotas(TILE)
    return jnp.sum(jnp.where(r == c, tile.astype(F32), 0.0), axis=0, keepdims=True)


def pack(packet, cov, start, passenger, chunk):
    rows, n = cov.shape
    paired = packet.shape[1] == rows
    row = lax.broadcasted_iota(jnp.int32, (SPARE, TILE if paired else n), 0)
    if not paired:
        packet[:rows, :] = cov[...]
        packet[rows:, :] = jnp.where(row == 0, passenger[...], 0.0).astype(BF16)
        return
    size = packet.shape[0] - SPARE
    other = n - rows - start
    r, c = iotas(TILE)
    for k in range(0, size, TILE):
        i = chunk * size + k
        for j in range(0, rows, TILE):
            mine = cov[i : i + TILE, pl.ds(pl.multiple_of(start + j, TILE), TILE)]
            cross = cov[i : i + TILE, pl.ds(pl.multiple_of(other + j, TILE), TILE)]
            if j > i:
                tile = mine
            elif j < i:
                tile = cross
            else:
                tile = jnp.where(c >= r, mine.astype(F32), cross.astype(F32)).astype(BF16)
                spare = jnp.where(row == 0, tile_diag(cross), 0.0)
                if passenger is not None:
                    for k_row in range(n // rows):
                        at = k_row * rows + i
                        spare = jnp.where(row == k_row + 1, passenger[:, at : at + TILE], spare)
                packet[size:, i : i + TILE] = spare.astype(BF16)
            packet[k : k + TILE, j : j + TILE] = tile


def unpack(full, diag, rider, packets, start, chunk):
    n = full.shape[0]
    if len(packets) == 1:
        (packet,) = packets
        rows = packet.shape[1] - SPARE
        for k in range(packet.shape[0]):
            full[k * rows : (k + 1) * rows, :] = packet[k, :rows, :]
        for i in range(0, n, TILE):
            diag[:, i : i + TILE] = tile_diag(full[i : i + TILE, i : i + TILE])
        rider[...] = packet[0, rows:, :].astype(F32)[0:1]
        return
    size = packets[0].shape[0] - SPARE
    rows = packets[0].shape[1]
    base = (start, n - rows - start)
    r, c = iotas(TILE)

    def put(at_row, i, at_col, j, tile):
        full[
            pl.ds(pl.multiple_of(at_row + i, TILE), TILE),
            pl.ds(pl.multiple_of(at_col + j, TILE), TILE),
        ] = tile

    for k in range(0, size, TILE):
        i = chunk * size + k
        spare = packets[0][size:, i : i + TILE].astype(F32)
        for k_row in range(n // rows):
            at = k_row * rows + i
            rider[:, at : at + TILE] = spare[k_row + 1 : k_row + 2]
        for mine, yours in ((0, 1), (1, 0)):
            for j in range(0, rows, TILE):
                tile = packets[mine][k : k + TILE, j : j + TILE]
                flip = tile.T
                if j > i:
                    put(base[mine], i, base[mine], j, tile)
                    put(base[mine], j, base[mine], i, flip)
                elif j < i:
                    put(base[mine], i, base[yours], j, tile)
                    put(base[yours], j, base[mine], i, flip)
                else:
                    tile = tile.astype(F32)
                    flip = flip.astype(F32)
                    theirs = packets[yours][k : k + TILE, i : i + TILE].T.astype(F32)
                    own = jnp.where(c >= r, tile, flip)
                    put(base[mine], i, base[mine], i, own.astype(BF16))
                    cross = jnp.where(c < r, tile, jnp.where(c > r, theirs, spare[0:1]))
                    put(base[mine], i, base[yours], i, cross.astype(BF16))
                    diag[:, pl.ds(pl.multiple_of(base[mine] + i, TILE), TILE)] = tile_diag(own)


def product_rows(cov, gram, left, at, right, chunk, chunks):
    size = cov.shape[0] // chunks
    row = chunk * size
    here = pl.ds(pl.multiple_of(at + row, size), size)
    term = mm_t(left[:, here], right[...])
    cov[row : row + size, :] = (gram[row : row + size, :] + term).astype(BF16)


def strips(rows):
    return [(k * TILE, (k + 1) * TILE, k * (k + 1) // 2 * TILE) for k in range(rows // TILE)]


def fold_kernel(ids, factor, lower, own, lower_a, lower_b, square, cross, sems):
    rows = factor.shape[0]
    cut = lower_a.shape[0]
    start = pl.multiple_of(ids[0], rows)
    moves = [(factor, own)]
    for row, width, at in strips(rows):
        moves.append(
            (factor.at[row : row + TILE, pl.ds(start, width)], square.at[:, at : at + width])
        )
    moves += [
        (lower.at[:cut], lower_a),
        (lower.at[cut:], lower_b),
        (factor.at[:, :rows], cross),
    ]
    copies = [pltpu.make_async_copy(s, t, sems.at[i]) for i, (s, t) in enumerate(moves)]
    for copy in copies:
        copy.start()
    for copy in copies:
        copy.wait()


def unfold(target, squares, crosses, start, sems):
    n = target.shape[0]
    rows = n // 2
    moves = []
    for square, base in zip(squares, (start, n - rows - start)):
        for row, width, at in strips(rows):
            here = pl.ds(pl.multiple_of(base + row, TILE), TILE)
            cols = pl.ds(pl.multiple_of(base, rows), width)
            moves.append((square.at[:, at : at + width], target.at[here, cols]))
            if width < rows:
                rest = pl.ds(pl.multiple_of(base + width, TILE), rows - width)
                target[here, rest] = jnp.zeros((TILE, rows - width), BF16)
    target[:rows, rows:] = jnp.zeros((rows, n - rows), BF16)
    copies = [pltpu.make_async_copy(s, t, sems.at[i]) for i, (s, t) in enumerate(moves)]
    for copy in copies:
        copy.start()
    low = target.at[rows:, :rows]

    @pl.when(start == 0)
    def _():
        pltpu.make_async_copy(crosses[1], low, sems.at[len(moves)]).start()

    @pl.when(start != 0)
    def _():
        pltpu.make_async_copy(crosses[0], low, sems.at[len(moves)]).start()

    return copies + [pltpu.make_async_copy(crosses[0], low, sems.at[len(moves)])]


def place(target, pieces, start):
    n = target.shape[0]
    if len(pieces) == 1:
        target[...] = pieces[0][...]
        return
    rows = pieces[0].shape[0]
    for piece, at in zip(pieces, (start, n - rows - start)):
        target[pl.ds(pl.multiple_of(at, rows), rows), :] = piece[...]


def gram_kernel(pieces, ids, *refs):
    pieces, (factor, gram) = refs[:pieces], refs[pieces:]
    rows, n = gram.shape
    half = n // 2
    start = pl.multiple_of(ids[0], rows)
    own = pl.ds(start, rows)
    place(factor, pieces, start)
    gram[:, :half] = mm_t(factor[:, own], factor[:, :half])
    gram[:, half:] = mm_t(factor[half:, own], factor[half:, half:])


def first_kernel(pieces, chunks, ids, *refs):
    lowers = refs[:pieces]
    factor, gram, coupling, packet, cov = refs[pieces:]
    rows, n = cov.shape
    start = pl.multiple_of(ids[0], rows)
    if pieces == 1:
        placed = [(lowers[0], 0)]
    else:
        first, second, other = lowers
        placed = [
            (first, start),
            (second, pl.multiple_of(start + first.shape[0], TILE)),
            (other, pl.multiple_of(n - rows - start, rows)),
        ]
    couple(coupling, placed, factor)

    @pl.when(ids[1] == TB - 1)
    def _():
        product_rows(cov, gram, coupling, start, coupling, 0, chunks)
        pack(packet, cov, start, None if chunks > 1 else jnp.zeros((1, n), F32), 0)


def rest_kernel(block, ids, gram, coupling, *refs):
    packet, cov = refs[len(refs) - 2 :]
    start = pl.multiple_of(ids[0], cov.shape[0])
    left, at, passenger = coupling, start, None
    if len(refs) > 3:
        left, at, passenger = refs[0], 0, refs[1]

    @pl.when(ids[1] == block)
    def _():
        product_rows(cov, gram, left, at, coupling, 1, 2)
        pack(packet, cov, start, passenger, 1)


def open_kernel(lowest, highest, ids, mine, yours, full, diag, rider):
    @pl.when(jnp.logical_and(ids[1] >= lowest, ids[1] <= highest))
    def _():
        unpack(full, diag, rider, (mine, yours), ids[0], 0)


def second_kernel(pieces, chunks, ids, *refs):
    packets = refs[:pieces]
    coupling, gram = refs[pieces : pieces + 2]
    packet, half, cov, full, diag, rider = refs[len(refs) - 6 :]
    rows = cov.shape[0]
    start = pl.multiple_of(ids[0], rows)

    @pl.when(ids[1] == TB - 2)
    def _():
        unpack(full, diag, rider, packets, start, chunks - 1)
        half[...] = mm(full[...], coupling[:, pl.ds(start, rows)]).astype(BF16)
        product_rows(cov, gram, half, 0, coupling, 0, chunks)
        pack(packet, cov, start, diag, 0)


def heard_kernel(parts, ids, *refs):
    parts, rest = refs[:parts], refs[parts:]
    (factor, coupling, cov_3, full_2, cov_2, heard, gram_1, diag_0, coupling_1, coupling_0,
     off_out, cov_out, off, sems, out_sems) = rest
    rows, _ = cov_3.shape
    start = pl.multiple_of(ids[0], rows)
    block = ids[1]

    @pl.when(block == TB - 1)
    def _():
        off[...] = -coupling[pl.ds(start, rows), :]
        write_out((off, cov_3), (off_out, cov_out), out_sems)

    @pl.when(block == TB - 2)
    def _():
        off[...] = (-mm(full_2[pl.ds(start, rows), :], coupling[...])).astype(BF16)
        write_out((off, cov_2), (off_out, cov_out), out_sems)

    def finish(factor_1, factor_0, known):
        known[...] = coupling[...]
        gram_1[...] = mm_t(factor_1[:, pl.ds(start, rows)], factor_1[...])
        diag_0[...] = jnp.sum(jnp.square(factor_0[...].astype(F32)), axis=0, keepdims=True)

    @pl.when(block < 2)
    def _():
        if len(parts) > 1:
            for copy in unfold(heard, parts[:2], parts[2:], start, sems):
                copy.wait()
        else:
            heard[...] = parts[0][...]

        @pl.when(block == 0)
        def _():
            finish(heard, factor, coupling_0)

        @pl.when(block == 1)
        def _():
            finish(factor, heard, coupling_1)


def ready_kernel(pieces, rows, first, ids, *refs):
    lowers, heard = refs[:pieces], refs[pieces]
    coupling_1, coupling_0 = refs[len(refs) - 2 :]
    n = heard.shape[0]
    placed = [(lowers[0], 0)]
    if pieces > 1:
        bases = (ids[0], n - rows - ids[0])
        placed = [(p, pl.multiple_of(b + first, TILE)) for p, b in zip(lowers, bases)]

    @pl.when(ids[1] == 0)
    def _():
        couple(coupling_1, placed, heard)

    @pl.when(ids[1] == 1)
    def _():
        couple(coupling_0, placed, heard)


def merge_kernel(ids, at_0, at_1, out, sem):
    block = ids[1]

    @pl.when(block == 0)
    def _():
        copy = pltpu.make_async_copy(at_0, out, sem.at[0])
        copy.start()
        copy.wait()

    @pl.when(block == 1)
    def _():
        copy = pltpu.make_async_copy(at_1, out, sem.at[0])
        copy.start()
        copy.wait()


def third_kernel(pieces, chunks, ids, *refs):
    packets = refs[:pieces]
    coupling_1, gram_1, coupling_0 = refs[pieces : pieces + 3]
    off_0, cov_1, sums, full, diag, rider, half = refs[len(refs) - 7 :]
    rows, _ = cov_1.shape
    start = pl.multiple_of(ids[0], rows)
    own = pl.ds(start, rows)

    @pl.when(ids[1] < 2)
    def _():
        unpack(full, diag, rider, packets, start, chunks - 1)
        half[...] = mm(full[...], coupling_1[:, own]).astype(BF16)
        product_rows(cov_1, gram_1, half, 0, coupling_1, 0, 1)
        off_0[...] = (-mm(cov_1[...], coupling_0[...])).astype(BF16)
        product = coupling_0[own, :].astype(F32) * off_0[...].astype(F32)
        sums[...] = jnp.zeros(sums.shape, F32)
        sums[0:1, :] = jnp.sum(product, axis=0, keepdims=True)
        for i in range(0, rows, TILE):
            at = pl.ds(pl.multiple_of(start + i, TILE), TILE)
            sums[1:2, at] = tile_diag(cov_1[i : i + TILE, at])


def combine_kernel(ids, *refs):
    diag_0, var_2, var_3, variances = refs[len(refs) - 4 :]
    parts = refs[: len(refs) - 4]

    @pl.when(ids[1] < 2)
    def _():
        if len(parts) > 1:
            total = parts[0][...] + parts[1][...]
        else:
            total = jnp.sum(parts[0][...], axis=0)
        row = lax.broadcasted_iota(jnp.int32, variances.shape, 0)
        values = jnp.where(row == 0, diag_0[...] - total[0:1], total[1:2])
        values = jnp.where(row == 2, var_2[...], jnp.where(row == 3, var_3[...], values))
        variances[...] = values.astype(BF16)


def owned_lines(mask, variances):
    values = variances[...].astype(F32)
    lines = []
    for slot in range(SLOTS):
        line = jnp.zeros((1, values.shape[1]), F32)
        for t in range(TB):
            at = slot * TB + t
            line += jnp.where(mask[at : at + 1, :] > 0, values[t : t + 1], 0.0)
        lines.append(line)
    return lines


def choose_kernel(ids, owner, mask):
    for t in range(TB):
        rank = jnp.int32(0)
        for before in range(t):
            rank += (owner[before] == owner[t]).astype(jnp.int32)
        for slot in range(SLOTS):
            here = jnp.logical_and(owner[t] == ids[2], rank == slot)
            at = slot * TB + t
            mask[at : at + 1, :] = jnp.full((1, mask.shape[1]), jnp.where(here, 1.0, 0.0), F32)


def last_kernel(pieces, ids, *refs):
    offs, refs = refs[:pieces], refs[pieces:]
    (coupling_0, gram, off_0, full, coupling_1, cov_1, variances, mask, _, _,
     off_out, cov_out, own_out, cov, off_1, lines, sems) = refs
    rows, n = cov.shape
    start = pl.multiple_of(ids[0], rows)
    block = ids[1]
    own = pl.ds(start, rows)

    def begin(source, target, sem):
        copy = pltpu.make_async_copy(source, target, sems.at[sem])
        copy.start()
        return copy

    def owned():
        for slot, line in enumerate(owned_lines(mask, variances)):
            lines[slot : slot + 1, :] = line
        return begin(lines, own_out, 0)

    @pl.when(block == 1)
    def _():
        copies = [begin(cov_1, cov_out, 1), owned()]
        off_1[...] = (-mm(full[own, :], coupling_1[...])).astype(BF16)
        copies.append(begin(off_1, off_out, 2))
        for copy in copies:
            copy.wait()

    @pl.when(block == 0)
    def _():
        copies = [begin(off_0, off_out, 1), owned()]
        parts = 2 if rows % (2 * TILE) == 0 else 1
        size = rows // parts
        bases = (start, n - rows - start) if pieces > 1 else (0,)
        for k in range(parts):
            cols = pl.ds(pl.multiple_of(start + k * size, size), size)
            total = gram[k * size : (k + 1) * size, :]
            for off, base in zip(offs, bases):
                here = pl.ds(pl.multiple_of(base, rows), off.shape[0])
                total -= mm_t(coupling_0[here, cols], off[...])
            here = pl.ds(k * size, size)
            cov[here, :] = total.astype(BF16)
            copies.append(begin(cov.at[here], cov_out.at[here], k + 2))
        for copy in copies:
            copy.wait()


def deliver_kernel(ids, mask, heard, _, own_out, lines, sems):
    @pl.when(ids[1] >= 2)
    def _():
        for slot, line in enumerate(owned_lines(mask, heard)):
            lines[slot : slot + 1, :] = line
        copy = pltpu.make_async_copy(lines, own_out, sems.at[0])
        copy.start()
        copy.wait()


def shards(linv, sub, owner):
    group = lax.axis_size("tm") // TB
    rows, n = linv.shape
    paired = group == 2
    dev = lax.axis_index("tm")
    member = dev % group

    def block_to_block(values, routes, members=range(group)):
        pairs = [(s * group + i, t * group + i) for s, t in routes for i in members]
        return lax.ppermute(values, "tm", pairs)

    def peer(piece, step=1):
        return lax.ppermute(piece, "tm", [(i, i ^ step) for i in range(TB * group)])

    def pieces_of(piece):
        if paired:
            return [piece, peer(piece)]
        step = 1
        while step < group:
            other = peer(piece, step)
            upper = (member // step) % 2 == 1
            piece = jnp.concatenate(
                [jnp.where(upper, other, piece), jnp.where(upper, piece, other)], 0
            )
            step *= 2
        return [piece]

    def packets_of(packet):
        return pieces_of(packet) if paired else pieces_of(packet[None])

    def after(values, *others):
        return lax.optimization_barrier((values, *others))[0]

    def call(kernel, out, inputs, spaces, scratch, aliases=None):
        shapes = tuple(
            pltpu.HBM(o[1], o[2]) if o[0] is HBM else pltpu.VMEM(o[1], o[2]) for o in out
        )
        placed = [
            x if space is SMEM else pltpu.with_memory_space_constraint(x, space.memory_space)
            for x, space in zip(inputs, spaces, strict=True)
        ]
        return pl.pallas_call(
            located(kernel, rows, group),
            out_shape=shapes,
            in_specs=list(spaces),
            out_specs=tuple(o[0] for o in out),
            scratch_shapes=scratch,
            input_output_aliases=aliases or {},
            compiler_params=PARAMS,
        )(*placed)

    def sems(*shape):
        return pltpu.SemaphoreType.DMA(shape)

    pieces = 2 if paired else 1
    chunks = 2 if paired else 1
    size = rows // chunks
    packet_shape = (size + SPARE, rows if paired else n)
    whole = (VMEM, (n, n), BF16)
    part = (VMEM, (rows, n), BF16)
    tall = (VMEM, (n, rows), BF16)
    line = (VMEM, (1, n), F32)
    packed = (VMEM, packet_shape, BF16)
    out_rows = (HBM, (rows, n), BF16)

    def swapped(piece, *others):
        return pieces_of(after(piece, *others) if others else piece)

    swap = [(1, 0), (0, 1)]
    if paired:
        other_factor, other_lower = peer(linv), peer(sub)
        cut = rows // 2
        own, lower_a, lower_b, square, cross = call(
            fold_kernel,
            [part, (VMEM, (cut, n), BF16), (VMEM, (rows - cut, n), BF16),
             (VMEM, (TILE, sum(w for _, w, _ in strips(rows))), BF16),
             (VMEM, (rows, rows), BF16)],
            [linv, sub],
            [HBM, HBM],
            [sems(4 + len(strips(rows)))],
        )
        factors = [own, other_factor]
        lowers = [lower_a, lower_b, other_lower]
        raw_lower = [block_to_block(lower_a, swap), block_to_block(lower_b, swap)]
        raw_factor = [block_to_block(square, swap), block_to_block(cross, swap, range(1, 2))]
    else:
        factors = pieces_of(linv)
        lowers = pieces_of(sub)
        raw_lower = [block_to_block(sub, swap)]
        raw_factor = [block_to_block(linv, swap)]

    factor, gram = call(
        functools.partial(gram_kernel, pieces),
        [whole, (VMEM, (rows, n), F32)],
        [*factors],
        [VMEM] * pieces,
        [],
    )
    coupling, packet_a, cov_3 = call(
        functools.partial(first_kernel, len(lowers), chunks),
        [whole, packed, part],
        [*lowers, factor, gram],
        [VMEM] * (len(lowers) + 2),
        [],
    )
    packets_2 = [block_to_block(packet_a, [(3, 2)])]
    if chunks > 1:
        packet_b, cov_3 = call(
            functools.partial(rest_kernel, TB - 1),
            [packed, part],
            [gram, coupling, cov_3],
            [VMEM] * 3,
            [],
            {2: 1},
        )
        packets_2.append(block_to_block(packet_b, [(3, 2)]))

    (mask,) = call(choose_kernel, [(VMEM, (SLOTS * TB, n), F32)], [owner], [SMEM], [])

    opened = []
    if chunks > 1:
        opened = call(
            functools.partial(open_kernel, 2, 2),
            [whole, line, line],
            [*packets_of(packets_2[0])],
            [VMEM, VMEM],
            [],
        )
    packet_a, half_2, cov_2, full_2, diag_2, _ = call(
        functools.partial(second_kernel, pieces, chunks),
        [packed, tall, part, whole, line, line],
        [*packets_of(packets_2[-1]), coupling, gram, *opened],
        [VMEM] * (pieces + 2 + len(opened)),
        [],
        {pieces + 2 + i: 3 + i for i in range(len(opened))},
    )
    packet = packet_a
    packets_0 = [block_to_block(packet_a, [(2, 0)])]
    packets_1 = [block_to_block(packet_a, [(2, 1)])]
    if chunks > 1:
        packet, cov_2 = call(
            functools.partial(rest_kernel, TB - 2),
            [packed, part],
            [gram, coupling, half_2, diag_2, cov_2],
            [VMEM] * 5,
            [],
            {4: 1},
        )
        packets_0.append(block_to_block(packet, [(2, 0)]))
        packets_1.append(block_to_block(packet, [(2, 1)]))

    parts = [x for piece in raw_factor for x in swapped(piece, packet)]
    heard_factor, gram_1, diag_0, coupling_1, coupling_0, off_rows, cov_rows = call(
        functools.partial(heard_kernel, len(parts)),
        [whole, (VMEM, (rows, n), F32), line, whole, whole, out_rows, out_rows],
        [*parts, factor, coupling, cov_3, full_2, cov_2],
        [VMEM] * (len(parts) + 5),
        [pltpu.VMEM((rows, n), BF16), sems(2 * (rows // TILE) + 1), sems(2)],
    )
    for k, piece in enumerate(raw_lower):
        coupling_1, coupling_0 = call(
            functools.partial(ready_kernel, pieces, rows, k * rows // 2),
            [whole, whole],
            [*swapped(piece, packet), heard_factor,
             coupling_1, coupling_0],
            [VMEM] * (pieces + 3),
            [],
            {pieces + 1: 0, pieces + 2: 1},
        )

    carried = [
        call(merge_kernel, [packed], [at_0, at_1], [VMEM, VMEM], [sems(1)])[0]
        for at_0, at_1 in zip(packets_0, packets_1)
    ]
    opened = []
    if chunks > 1:
        opened = call(
            functools.partial(open_kernel, 0, 1),
            [whole, line, line],
            [*packets_of(carried[0])],
            [VMEM, VMEM],
            [],
        )
    off_0, cov_1, sums, full_1, var_2, var_3, _ = call(
        functools.partial(third_kernel, pieces, chunks),
        [part, part, (VMEM, (8, n), F32), whole, line, line, tall],
        [*packets_of(carried[-1]), coupling_1, gram_1, coupling_0, *opened],
        [VMEM] * (pieces + 3 + len(opened)),
        [],
        {pieces + 3 + i: 3 + i for i in range(len(opened))},
    )
    offs = swapped(off_0)
    parts = packets_of(sums)
    (variances,) = call(
        combine_kernel,
        [(VMEM, (SPARE, n), BF16)],
        [*parts, diag_0, var_2, var_3],
        [VMEM] * (len(parts) + 3),
        [],
    )
    heard = block_to_block(variances, [(0, 2), (1, 3)])

    own_rows = (HBM, (SLOTS, n), F32)
    lines = pltpu.VMEM((SLOTS, n), F32)
    off_rows, cov_rows, owned_var = call(
        functools.partial(last_kernel, len(offs)),
        [out_rows, out_rows, own_rows],
        [*offs, coupling_0, gram, off_0, full_1, coupling_1, cov_1, variances, mask,
         off_rows, cov_rows],
        [VMEM] * (len(offs) + 8) + [HBM, HBM],
        [pltpu.VMEM((rows, n), BF16), pltpu.VMEM((rows, n), BF16), lines, sems(4)],
        {len(offs) + 8: 0, len(offs) + 9: 1},
    )
    (owned_var,) = call(
        deliver_kernel,
        [own_rows],
        [mask, heard, owned_var],
        [VMEM, VMEM, HBM],
        [lines, sems(1)],
        {2: 0},
    )
    return (cov_rows, off_rows, owned_var)


def solution(mesh):
    return jax.shard_map(
        shards,
        mesh=mesh,
        in_specs=(P(("cfg", "tm"), None), P(("cfg", "tm"), None), P("cfg")),
        out_specs=(P(("cfg", "tm"), None), P(("cfg", "tm"), None), P(("cfg", "tm"), None)),
        check_vma=False,
    )
```

```python
import functools

import jax
import jax.numpy as jnp
from jax import lax
from jax.experimental import pallas as pl
from jax.experimental.pallas import tpu as pltpu
from jax.sharding import PartitionSpec as P


TB = 4
SLOTS = 2
SPARE = 16
TILE = 128

CONTRACT_FIRST = (((0,), (0,)), ((), ()))
BF16 = jnp.bfloat16
F32 = jnp.float32

HBM = pl.BlockSpec(memory_space=pltpu.HBM)
VMEM = pl.BlockSpec(memory_space=pltpu.VMEM)
SMEM = pl.BlockSpec(memory_space=pltpu.SMEM)
PARAMS = pltpu.CompilerParams(vmem_limit_bytes=18 << 20)


def located(kernel, rows, group):
    def body(*refs):
        dev = lax.axis_index("tm")
        member = lax.rem(dev, jnp.int32(group))
        kernel((member * rows, lax.div(dev, jnp.int32(group)), dev), *refs)

    return body


def mm(a, b):
    return jnp.dot(a, b, preferred_element_type=F32)


def mm_t(a, b):
    return lax.dot_general(a, b, CONTRACT_FIRST, preferred_element_type=F32)


def iotas(size):
    r = lax.broadcasted_iota(jnp.int32, (size, size), 0)
    c = lax.broadcasted_iota(jnp.int32, (size, size), 1)
    return r, c


def couple(target, lowers, factor):
    half = factor.shape[0] // 2
    for lower, at in lowers:
        here = pl.ds(at, lower.shape[0])
        target[here, :half] = mm(lower[...], factor[:, :half]).astype(BF16)
        target[here, half:] = mm(lower[:, half:], factor[half:, half:]).astype(BF16)


def write_out(values, outs, sems):
    copies = [
        pltpu.make_async_copy(v, o, sems.at[i]) for i, (v, o) in enumerate(zip(values, outs))
    ]
    for copy in copies:
        copy.start()
    for copy in copies:
        copy.wait()


def tile_diag(tile):
    r, c = iotas(TILE)
    return jnp.sum(jnp.where(r == c, tile.astype(F32), 0.0), axis=0, keepdims=True)


def pack(packet, cov, start, passenger, chunk):
    rows, n = cov.shape
    paired = packet.shape[1] == rows
    row = lax.broadcasted_iota(jnp.int32, (SPARE, TILE if paired else n), 0)
    if not paired:
        packet[:rows, :] = cov[...]
        packet[rows:, :] = jnp.where(row == 0, passenger[...], 0.0).astype(BF16)
        return
    size = packet.shape[0] - SPARE
    other = n - rows - start
    r, c = iotas(TILE)
    for k in range(0, size, TILE):
        i = chunk * size + k
        for j in range(0, rows, TILE):
            mine = cov[i : i + TILE, pl.ds(pl.multiple_of(start + j, TILE), TILE)]
            cross = cov[i : i + TILE, pl.ds(pl.multiple_of(other + j, TILE), TILE)]
            if j > i:
                tile = mine
            elif j < i:
                tile = cross
            else:
                tile = jnp.where(c >= r, mine.astype(F32), cross.astype(F32)).astype(BF16)
                spare = jnp.where(row == 0, tile_diag(cross), 0.0)
                if passenger is not None:
                    for k_row in range(n // rows):
                        at = k_row * rows + i
                        spare = jnp.where(row == k_row + 1, passenger[:, at : at + TILE], spare)
                packet[size:, i : i + TILE] = spare.astype(BF16)
            packet[k : k + TILE, j : j + TILE] = tile


def unpack(full, diag, rider, packets, start, chunk):
    n = full.shape[0]
    if len(packets) == 1:
        (packet,) = packets
        rows = packet.shape[1] - SPARE
        for k in range(packet.shape[0]):
            full[k * rows : (k + 1) * rows, :] = packet[k, :rows, :]
        for i in range(0, n, TILE):
            diag[:, i : i + TILE] = tile_diag(full[i : i + TILE, i : i + TILE])
        rider[...] = packet[0, rows:, :].astype(F32)[0:1]
        return
    size = packets[0].shape[0] - SPARE
    rows = packets[0].shape[1]
    base = (start, n - rows - start)
    r, c = iotas(TILE)

    def put(at_row, i, at_col, j, tile):
        full[
            pl.ds(pl.multiple_of(at_row + i, TILE), TILE),
            pl.ds(pl.multiple_of(at_col + j, TILE), TILE),
        ] = tile

    for k in range(0, size, TILE):
        i = chunk * size + k
        spare = packets[0][size:, i : i + TILE].astype(F32)
        for k_row in range(n // rows):
            at = k_row * rows + i
            rider[:, at : at + TILE] = spare[k_row + 1 : k_row + 2]
        for mine, yours in ((0, 1), (1, 0)):
            for j in range(0, rows, TILE):
                tile = packets[mine][k : k + TILE, j : j + TILE]
                flip = tile.T
                if j > i:
                    put(base[mine], i, base[mine], j, tile)
                    put(base[mine], j, base[mine], i, flip)
                elif j < i:
                    put(base[mine], i, base[yours], j, tile)
                    put(base[yours], j, base[mine], i, flip)
                else:
                    tile = tile.astype(F32)
                    flip = flip.astype(F32)
                    theirs = packets[yours][k : k + TILE, i : i + TILE].T.astype(F32)
                    own = jnp.where(c >= r, tile, flip)
                    put(base[mine], i, base[mine], i, own.astype(BF16))
                    cross = jnp.where(c < r, tile, jnp.where(c > r, theirs, spare[0:1]))
                    put(base[mine], i, base[yours], i, cross.astype(BF16))
                    diag[:, pl.ds(pl.multiple_of(base[mine] + i, TILE), TILE)] = tile_diag(own)


def product_rows(cov, gram, left, at, right, chunk, chunks):
    size = cov.shape[0] // chunks
    row = chunk * size
    here = pl.ds(pl.multiple_of(at + row, size), size)
    term = mm_t(left[:, here], right[...])
    cov[row : row + size, :] = (gram[row : row + size, :] + term).astype(BF16)


def strips(rows):
    return [(k * TILE, (k + 1) * TILE, k * (k + 1) // 2 * TILE) for k in range(rows // TILE)]


def fold_kernel(ids, factor, lower, own, lower_a, lower_b, square, cross, sems):
    rows = factor.shape[0]
    cut = lower_a.shape[0]
    start = pl.multiple_of(ids[0], rows)
    moves = [(factor, own)]
    for row, width, at in strips(rows):
        moves.append(
            (factor.at[row : row + TILE, pl.ds(start, width)], square.at[:, at : at + width])
        )
    moves += [
        (lower.at[:cut], lower_a),
        (lower.at[cut:], lower_b),
        (factor.at[:, :rows], cross),
    ]
    copies = [pltpu.make_async_copy(s, t, sems.at[i]) for i, (s, t) in enumerate(moves)]
    for copy in copies:
        copy.start()
    for copy in copies:
        copy.wait()


def unfold(target, squares, crosses, start, sems):
    n = target.shape[0]
    rows = n // 2
    moves = []
    for square, base in zip(squares, (start, n - rows - start)):
        for row, width, at in strips(rows):
            here = pl.ds(pl.multiple_of(base + row, TILE), TILE)
            cols = pl.ds(pl.multiple_of(base, rows), width)
            moves.append((square.at[:, at : at + width], target.at[here, cols]))
            if width < rows:
                rest = pl.ds(pl.multiple_of(base + width, TILE), rows - width)
                target[here, rest] = jnp.zeros((TILE, rows - width), BF16)
    target[:rows, rows:] = jnp.zeros((rows, n - rows), BF16)
    copies = [pltpu.make_async_copy(s, t, sems.at[i]) for i, (s, t) in enumerate(moves)]
    for copy in copies:
        copy.start()
    low = target.at[rows:, :rows]

    @pl.when(start == 0)
    def _():
        pltpu.make_async_copy(crosses[1], low, sems.at[len(moves)]).start()

    @pl.when(start != 0)
    def _():
        pltpu.make_async_copy(crosses[0], low, sems.at[len(moves)]).start()

    return copies + [pltpu.make_async_copy(crosses[0], low, sems.at[len(moves)])]


def place(target, pieces, start):
    n = target.shape[0]
    if len(pieces) == 1:
        target[...] = pieces[0][...]
        return
    rows = pieces[0].shape[0]
    for piece, at in zip(pieces, (start, n - rows - start)):
        target[pl.ds(pl.multiple_of(at, rows), rows), :] = piece[...]


def gram_kernel(pieces, ids, *refs):
    pieces, (factor, gram) = refs[:pieces], refs[pieces:]
    rows, n = gram.shape
    half = n // 2
    start = pl.multiple_of(ids[0], rows)
    own = pl.ds(start, rows)
    place(factor, pieces, start)
    gram[:, :half] = mm_t(factor[:, own], factor[:, :half])
    gram[:, half:] = mm_t(factor[half:, own], factor[half:, half:])


def first_kernel(pieces, chunks, ids, *refs):
    lowers = refs[:pieces]
    factor, gram, coupling, packet, cov = refs[pieces:]
    rows, n = cov.shape
    start = pl.multiple_of(ids[0], rows)
    if pieces == 1:
        placed = [(lowers[0], 0)]
    else:
        first, second, other = lowers
        placed = [
            (first, start),
            (second, pl.multiple_of(start + first.shape[0], TILE // 2)),
            (other, pl.multiple_of(n - rows - start, rows)),
        ]
    couple(coupling, placed, factor)

    @pl.when(ids[1] == TB - 1)
    def _():
        product_rows(cov, gram, coupling, start, coupling, 0, chunks)
        pack(packet, cov, start, None if chunks > 1 else jnp.zeros((1, n), F32), 0)


def rest_kernel(block, ids, gram, coupling, *refs):
    packet, cov = refs[len(refs) - 2 :]
    start = pl.multiple_of(ids[0], cov.shape[0])
    left, at, passenger = coupling, start, None
    if len(refs) > 3:
        left, at, passenger = refs[0], 0, refs[1]

    @pl.when(ids[1] == block)
    def _():
        product_rows(cov, gram, left, at, coupling, 1, 2)
        pack(packet, cov, start, passenger, 1)


def open_kernel(lowest, highest, ids, mine, yours, full, diag, rider):
    @pl.when(jnp.logical_and(ids[1] >= lowest, ids[1] <= highest))
    def _():
        unpack(full, diag, rider, (mine, yours), ids[0], 0)


def second_kernel(pieces, chunks, ids, *refs):
    packets = refs[:pieces]
    coupling, gram = refs[pieces : pieces + 2]
    packet, half, cov, full, diag, rider = refs[len(refs) - 6 :]
    rows = cov.shape[0]
    start = pl.multiple_of(ids[0], rows)

    @pl.when(ids[1] == TB - 2)
    def _():
        unpack(full, diag, rider, packets, start, chunks - 1)
        half[...] = mm(full[...], coupling[:, pl.ds(start, rows)]).astype(BF16)
        product_rows(cov, gram, half, 0, coupling, 0, chunks)
        pack(packet, cov, start, diag, 0)


def heard_kernel(parts, ids, *refs):
    parts, rest = refs[:parts], refs[parts:]
    (factor, coupling, cov_3, full_2, cov_2, heard, gram_1, diag_0, coupling_1, coupling_0,
     off_out, cov_out, off, sems, out_sems) = rest
    rows, _ = cov_3.shape
    start = pl.multiple_of(ids[0], rows)
    block = ids[1]

    @pl.when(block == TB - 1)
    def _():
        off[...] = -coupling[pl.ds(start, rows), :]
        write_out((off, cov_3), (off_out, cov_out), out_sems)

    @pl.when(block == TB - 2)
    def _():
        off[...] = (-mm(full_2[pl.ds(start, rows), :], coupling[...])).astype(BF16)
        write_out((off, cov_2), (off_out, cov_out), out_sems)

    def finish(factor_1, factor_0, known):
        known[...] = coupling[...]
        gram_1[...] = mm_t(factor_1[:, pl.ds(start, rows)], factor_1[...])
        diag_0[...] = jnp.sum(jnp.square(factor_0[...].astype(F32)), axis=0, keepdims=True)

    @pl.when(block < 2)
    def _():
        if len(parts) > 1:
            for copy in unfold(heard, parts[:2], parts[2:], start, sems):
                copy.wait()
        else:
            heard[...] = parts[0][...]

        @pl.when(block == 0)
        def _():
            finish(heard, factor, coupling_0)

        @pl.when(block == 1)
        def _():
            finish(factor, heard, coupling_1)


def ready_kernel(pieces, rows, first, ids, *refs):
    lowers, heard = refs[:pieces], refs[pieces]
    coupling_1, coupling_0 = refs[len(refs) - 2 :]
    n = heard.shape[0]
    placed = [(lowers[0], 0)]
    if pieces > 1:
        bases = (ids[0], n - rows - ids[0])
        placed = [(p, pl.multiple_of(b + first, TILE // 2)) for p, b in zip(lowers, bases)]

    @pl.when(ids[1] == 0)
    def _():
        couple(coupling_1, placed, heard)

    @pl.when(ids[1] == 1)
    def _():
        couple(coupling_0, placed, heard)


def merge_kernel(ids, at_0, at_1, out, sem):
    block = ids[1]

    @pl.when(block == 0)
    def _():
        copy = pltpu.make_async_copy(at_0, out, sem.at[0])
        copy.start()
        copy.wait()

    @pl.when(block == 1)
    def _():
        copy = pltpu.make_async_copy(at_1, out, sem.at[0])
        copy.start()
        copy.wait()


def third_kernel(pieces, chunks, ids, *refs):
    packets = refs[:pieces]
    coupling_1, gram_1, coupling_0 = refs[pieces : pieces + 3]
    off_0, cov_1, sums, full, diag, rider, half = refs[len(refs) - 7 :]
    rows, _ = cov_1.shape
    start = pl.multiple_of(ids[0], rows)
    own = pl.ds(start, rows)

    @pl.when(ids[1] < 2)
    def _():
        unpack(full, diag, rider, packets, start, chunks - 1)
        half[...] = mm(full[...], coupling_1[:, own]).astype(BF16)
        product_rows(cov_1, gram_1, half, 0, coupling_1, 0, 1)
        off_0[...] = (-mm(cov_1[...], coupling_0[...])).astype(BF16)
        product = coupling_0[own, :].astype(F32) * off_0[...].astype(F32)
        sums[...] = jnp.zeros(sums.shape, F32)
        sums[0:1, :] = jnp.sum(product, axis=0, keepdims=True)
        for i in range(0, rows, TILE):
            at = pl.ds(pl.multiple_of(start + i, TILE), TILE)
            sums[1:2, at] = tile_diag(cov_1[i : i + TILE, at])


def combine_kernel(ids, *refs):
    diag_0, var_2, var_3, variances = refs[len(refs) - 4 :]
    parts = refs[: len(refs) - 4]

    @pl.when(ids[1] < 2)
    def _():
        if len(parts) > 1:
            total = parts[0][...] + parts[1][...]
        else:
            total = jnp.sum(parts[0][...], axis=0)
        row = lax.broadcasted_iota(jnp.int32, variances.shape, 0)
        values = jnp.where(row == 0, diag_0[...] - total[0:1], total[1:2])
        values = jnp.where(row == 2, var_2[...], jnp.where(row == 3, var_3[...], values))
        variances[...] = values.astype(BF16)


def owned_lines(mask, variances):
    values = variances[...].astype(F32)
    lines = []
    for slot in range(SLOTS):
        line = jnp.zeros((1, values.shape[1]), F32)
        for t in range(TB):
            at = slot * TB + t
            line += jnp.where(mask[at : at + 1, :] > 0, values[t : t + 1], 0.0)
        lines.append(line)
    return lines


def choose_kernel(ids, owner, mask):
    for t in range(TB):
        rank = jnp.int32(0)
        for before in range(t):
            rank += (owner[before] == owner[t]).astype(jnp.int32)
        for slot in range(SLOTS):
            here = jnp.logical_and(owner[t] == ids[2], rank == slot)
            at = slot * TB + t
            mask[at : at + 1, :] = jnp.full((1, mask.shape[1]), jnp.where(here, 1.0, 0.0), F32)


def last_kernel(pieces, ids, *refs):
    offs, refs = refs[:pieces], refs[pieces:]
    (coupling_0, gram, off_0, full, coupling_1, cov_1, variances, mask, _, _,
     off_out, cov_out, own_out, cov, off_1, lines, sems) = refs
    rows, n = cov.shape
    start = pl.multiple_of(ids[0], rows)
    block = ids[1]
    own = pl.ds(start, rows)

    def begin(source, target, sem):
        copy = pltpu.make_async_copy(source, target, sems.at[sem])
        copy.start()
        return copy

    def owned():
        for slot, line in enumerate(owned_lines(mask, variances)):
            lines[slot : slot + 1, :] = line
        return begin(lines, own_out, 0)

    @pl.when(block == 1)
    def _():
        copies = [begin(cov_1, cov_out, 1), owned()]
        off_1[...] = (-mm(full[own, :], coupling_1[...])).astype(BF16)
        copies.append(begin(off_1, off_out, 2))
        for copy in copies:
            copy.wait()

    @pl.when(block == 0)
    def _():
        copies = [begin(off_0, off_out, 1), owned()]
        parts = 2 if rows % (2 * TILE) == 0 else 1
        size = rows // parts
        bases = (start, n - rows - start) if pieces > 1 else (0,)
        for k in range(parts):
            cols = pl.ds(pl.multiple_of(start + k * size, size), size)
            total = gram[k * size : (k + 1) * size, :]
            for off, base in zip(offs, bases):
                here = pl.ds(pl.multiple_of(base, rows), off.shape[0])
                total -= mm_t(coupling_0[here, cols], off[...])
            here = pl.ds(k * size, size)
            cov[here, :] = total.astype(BF16)
            copies.append(begin(cov.at[here], cov_out.at[here], k + 2))
        for copy in copies:
            copy.wait()


def deliver_kernel(ids, mask, heard, _, own_out, lines, sems):
    @pl.when(ids[1] >= 2)
    def _():
        for slot, line in enumerate(owned_lines(mask, heard)):
            lines[slot : slot + 1, :] = line
        copy = pltpu.make_async_copy(lines, own_out, sems.at[0])
        copy.start()
        copy.wait()


def shards(linv, sub, owner):
    group = lax.axis_size("tm") // TB
    rows, n = linv.shape
    paired = group == 2
    dev = lax.axis_index("tm")
    member = dev % group

    def block_to_block(values, routes, members=range(group)):
        pairs = [(s * group + i, t * group + i) for s, t in routes for i in members]
        return lax.ppermute(values, "tm", pairs)

    def peer(piece, step=1):
        return lax.ppermute(piece, "tm", [(i, i ^ step) for i in range(TB * group)])

    def pieces_of(piece):
        if paired:
            return [piece, peer(piece)]
        step = 1
        while step < group:
            other = peer(piece, step)
            upper = (member // step) % 2 == 1
            piece = jnp.concatenate(
                [jnp.where(upper, other, piece), jnp.where(upper, piece, other)], 0
            )
            step *= 2
        return [piece]

    def packets_of(packet):
        return pieces_of(packet) if paired else pieces_of(packet[None])

    def after(values, *others):
        return lax.optimization_barrier((values, *others))[0]

    def call(kernel, out, inputs, spaces, scratch, aliases=None):
        shapes = tuple(
            pltpu.HBM(o[1], o[2]) if o[0] is HBM else pltpu.VMEM(o[1], o[2]) for o in out
        )
        placed = [
            x if space is SMEM else pltpu.with_memory_space_constraint(x, space.memory_space)
            for x, space in zip(inputs, spaces, strict=True)
        ]
        return pl.pallas_call(
            located(kernel, rows, group),
            out_shape=shapes,
            in_specs=list(spaces),
            out_specs=tuple(o[0] for o in out),
            scratch_shapes=scratch,
            input_output_aliases=aliases or {},
            compiler_params=PARAMS,
        )(*placed)

    def sems(*shape):
        return pltpu.SemaphoreType.DMA(shape)

    pieces = 2 if paired else 1
    chunks = 2 if paired else 1
    size = rows // chunks
    packet_shape = (size + SPARE, rows if paired else n)
    whole = (VMEM, (n, n), BF16)
    part = (VMEM, (rows, n), BF16)
    tall = (VMEM, (n, rows), BF16)
    line = (VMEM, (1, n), F32)
    packed = (VMEM, packet_shape, BF16)
    out_rows = (HBM, (rows, n), BF16)

    def swapped(piece, *others):
        return pieces_of(after(piece, *others) if others else piece)

    swap = [(1, 0), (0, 1)]
    if paired:
        other_factor, other_lower = peer(linv), peer(sub)
        cut = rows // 2
        own, lower_a, lower_b, square, cross = call(
            fold_kernel,
            [part, (VMEM, (cut, n), BF16), (VMEM, (rows - cut, n), BF16),
             (VMEM, (TILE, sum(w for _, w, _ in strips(rows))), BF16),
             (VMEM, (rows, rows), BF16)],
            [linv, sub],
            [HBM, HBM],
            [sems(4 + len(strips(rows)))],
        )
        factors = [own, other_factor]
        lowers = [lower_a, lower_b, other_lower]
        raw_lower = [block_to_block(lower_a, swap), block_to_block(lower_b, swap)]
        raw_factor = [block_to_block(square, swap), block_to_block(cross, swap, range(1, 2))]
    else:
        factors = pieces_of(linv)
        lowers = pieces_of(sub)
        raw_lower = [block_to_block(sub, swap)]
        raw_factor = [block_to_block(linv, swap)]

    factor, gram = call(
        functools.partial(gram_kernel, pieces),
        [whole, (VMEM, (rows, n), F32)],
        [*factors],
        [VMEM] * pieces,
        [],
    )
    coupling, packet_a, cov_3 = call(
        functools.partial(first_kernel, len(lowers), chunks),
        [whole, packed, part],
        [*lowers, factor, gram],
        [VMEM] * (len(lowers) + 2),
        [],
    )
    packets_2 = [block_to_block(packet_a, [(3, 2)])]
    if chunks > 1:
        packet_b, cov_3 = call(
            functools.partial(rest_kernel, TB - 1),
            [packed, part],
            [gram, coupling, cov_3],
            [VMEM] * 3,
            [],
            {2: 1},
        )
        packets_2.append(block_to_block(packet_b, [(3, 2)]))

    (mask,) = call(choose_kernel, [(VMEM, (SLOTS * TB, n), F32)], [owner], [SMEM], [])

    opened = []
    if chunks > 1:
        opened = call(
            functools.partial(open_kernel, 2, 2),
            [whole, line, line],
            [*packets_of(packets_2[0])],
            [VMEM, VMEM],
            [],
        )
    packet_a, half_2, cov_2, full_2, diag_2, _ = call(
        functools.partial(second_kernel, pieces, chunks),
        [packed, tall, part, whole, line, line],
        [*packets_of(packets_2[-1]), coupling, gram, *opened],
        [VMEM] * (pieces + 2 + len(opened)),
        [],
        {pieces + 2 + i: 3 + i for i in range(len(opened))},
    )
    packet = packet_a
    packets_0 = [block_to_block(packet_a, [(2, 0)])]
    packets_1 = [block_to_block(packet_a, [(2, 1)])]
    if chunks > 1:
        packet, cov_2 = call(
            functools.partial(rest_kernel, TB - 2),
            [packed, part],
            [gram, coupling, half_2, diag_2, cov_2],
            [VMEM] * 5,
            [],
            {4: 1},
        )
        packets_0.append(block_to_block(packet, [(2, 0)]))
        packets_1.append(block_to_block(packet, [(2, 1)]))

    parts = [x for piece in raw_factor for x in swapped(piece, packet)]
    heard_factor, gram_1, diag_0, coupling_1, coupling_0, off_rows, cov_rows = call(
        functools.partial(heard_kernel, len(parts)),
        [whole, (VMEM, (rows, n), F32), line, whole, whole, out_rows, out_rows],
        [*parts, factor, coupling, cov_3, full_2, cov_2],
        [VMEM] * (len(parts) + 5),
        [pltpu.VMEM((rows, n), BF16), sems(2 * (rows // TILE) + 1), sems(2)],
    )
    for k, piece in enumerate(raw_lower):
        coupling_1, coupling_0 = call(
            functools.partial(ready_kernel, pieces, rows, k * rows // 2),
            [whole, whole],
            [*swapped(piece, packet), heard_factor,
             coupling_1, coupling_0],
            [VMEM] * (pieces + 3),
            [],
            {pieces + 1: 0, pieces + 2: 1},
        )

    carried = [
        call(merge_kernel, [packed], [at_0, at_1], [VMEM, VMEM], [sems(1)])[0]
        for at_0, at_1 in zip(packets_0, packets_1)
    ]
    opened = []
    if chunks > 1:
        opened = call(
            functools.partial(open_kernel, 0, 1),
            [whole, line, line],
            [*packets_of(carried[0])],
            [VMEM, VMEM],
            [],
        )
    off_0, cov_1, sums, full_1, var_2, var_3 = call(
        functools.partial(third_kernel, pieces, chunks),
        [part, part, (VMEM, (8, n), F32), whole, line, line],
        [*packets_of(carried[-1]), coupling_1, gram_1, coupling_0, *opened],
        [VMEM] * (pieces + 3 + len(opened)),
        [pltpu.VMEM((n, rows), BF16)],
        {pieces + 3 + i: 3 + i for i in range(len(opened))},
    )
    offs = swapped(off_0)
    parts = packets_of(sums)
    (variances,) = call(
        combine_kernel,
        [(VMEM, (SPARE, n), BF16)],
        [*parts, diag_0, var_2, var_3],
        [VMEM] * (len(parts) + 3),
        [],
    )
    heard = block_to_block(variances, [(0, 2), (1, 3)])

    own_rows = (HBM, (SLOTS, n), F32)
    lines = pltpu.VMEM((SLOTS, n), F32)
    off_rows, cov_rows, owned_var = call(
        functools.partial(last_kernel, len(offs)),
        [out_rows, out_rows, own_rows],
        [*offs, coupling_0, gram, off_0, full_1, coupling_1, cov_1, variances, mask,
         off_rows, cov_rows],
        [VMEM] * (len(offs) + 8) + [HBM, HBM],
        [pltpu.VMEM((rows, n), BF16), pltpu.VMEM((rows, n), BF16), lines, sems(4)],
        {len(offs) + 8: 0, len(offs) + 9: 1},
    )
    (owned_var,) = call(
        deliver_kernel,
        [own_rows],
        [mask, heard, owned_var],
        [VMEM, VMEM, HBM],
        [lines, sems(1)],
        {2: 0},
    )
    return (cov_rows, off_rows, owned_var)


def solution(mesh):
    return jax.shard_map(
        shards,
        mesh=mesh,
        in_specs=(P(("cfg", "tm"), None), P(("cfg", "tm"), None), P("cfg")),
        out_specs=(P(("cfg", "tm"), None), P(("cfg", "tm"), None), P(("cfg", "tm"), None)),
        check_vma=False,
    )
```
